32 devices in a mesh: section: 4 (over y, x), dom: 8 (over z, core).
Axes of the slice: x: 2, y: 2, z: 4, core: 2. Of those that a mesh axis runs over, the one named last changes fastest.
Arguments:
- source: float32 [4, 32, 2048], P('section', None, 'dom'), may hold values from -6 to 6
- initial: float32 [4, 2048], P('section', 'dom'), may hold values from -4 to 4
- capacitance: float32 [4, 2048], P('section', 'dom'), may hold values from 0.5 to 2
- block_matrix: float32 [4, 16, 128, 128], P('section', 'dom')
- block_inverse: float32 [4, 16, 128, 128], P('section', 'dom'), as said below
- net_weight: float32 [4, 2048, 512], P('section', 'dom'), may hold values from -0.125 to 0.125
- tap_nodes: int32 [4, 1024], P('section', 'dom'), may hold values from 0 to 255
- drive_nodes: int32 [4, 1024], P('section', 'dom'), may hold values from 0 to 255
- drive_gain: float32 [4, 1024], P('section', 'dom'), may hold values from 0.5 to 2
- attenuation: float32 [4, 1024], P('section', 'dom'), may hold values from 0 to 1
Outputs:
- waveform: float32 [4, 32, 2048], P('section', None, 'dom')
- mean_square: float32 [4], replicated
The draws below stay inside these ranges and needn't reach their ends.
Inputs may be any that keep to these rules, and one draw needn't show every extreme that they name: block_matrix holds symmetric positive definite blocks and block_inverse their inverses up to float32 rounding. `tap_nodes`: offsets within the device's own 256 nodes. `drive_nodes`: offsets within the device's own 256 nodes.
All inputs are finite; a program needn't handle non-finite values.
Results may differ from the reference program's by a relative error of at most 0.0001.
Values sent between devices are 32-bit elements; how exact they have to be, the bound alone decides.
No kernel may reach another device: no remote copies, remote signals or barrier semaphores. Data moves between devices by JAX's collectives and lax.ppermute only.
A program may use at most 64 MiB of HBM per device.

```python
import math
import jax
import jax.numpy as jnp
from jax import lax

STEPS = 32
BLOCK = 128
NET = 512
BND_DEV = 128
NEWTON = 2
SWEEPS = 2
SECTIONS = 4
NODES_DEV = 256
NODES = 2048
BLOCKS = 16
BND = 1024


def block_pair(key):
    inner = jax.random.fold_in(key, 4242)
    first, second = jax.random.split(inner)
    noise = jax.random.normal(first, (SECTIONS, BLOCKS, BLOCK, BLOCK), jnp.float32)
    noise = (noise + jnp.swapaxes(noise, 2, 3)) * (0.7071 / BLOCK ** 0.5)
    diagonal = jax.random.uniform(second, (SECTIONS, BLOCKS, BLOCK), jnp.float32, 3.0, 6.0)
    matrix = noise + diagonal[..., None] * jnp.eye(BLOCK, dtype=jnp.float32)
    return (matrix, jnp.linalg.inv(matrix))


def draw_block_matrix(key, part):
    return block_pair(key)[0]


def draw_block_inverse(key, part):
    return block_pair(key)[1]


def draw_attenuation(key, part):
    inner = jax.random.fold_in(key, 77)
    logs = jax.random.uniform(inner, (SECTIONS, BND), jnp.float32, -1.6, 2.1)
    rates = jnp.exp(logs)
    return jnp.exp(-rates * 1.2 / SECTIONS)


def plant(result, stream_key, least, high):
    shape = result.shape
    spot = [jax.random.randint(jax.random.fold_in(stream_key, axis), (), 0, shape[axis]) for axis in range(len(shape))]
    result = result.at[tuple(spot)].set(least)
    longest = shape.index(max(shape))
    spot[longest] = (spot[longest] + 1) % shape[longest]
    return result.at[tuple(spot)].set(high)


def shard_levels(own_key, dims, cuts, smallest, high):
    level = 1.0
    for dim, shards_of in cuts:
        steps = jax.random.uniform(jax.random.fold_in(jax.random.fold_in(own_key, 6), dim), (shards_of,), jnp.float32, smallest / len(cuts), high / len(cuts))
        level = level * jnp.repeat(jnp.exp(steps), dims[dim] // shards_of).reshape((-1,) + (1,) * (len(dims) - 1 - dim))
    return level


def normal_values(rng, extent, scale, limit, cuts=(), kind=jnp.bfloat16):
    values = scale * jax.random.normal(rng, extent, jnp.float32)
    if cuts:
        values = values * shard_levels(rng, extent, cuts, -0.22, 0.18)
    return jnp.clip(values, -limit, limit).astype(kind)


def setup_inputs(seed: int = 0) -> dict:
    seeds = jax.random.split(jax.random.key(seed), 11)
    source = normal_values(seeds[0], (SECTIONS, STEPS, NODES), 1.0, 6.0, ((0, 4), (2, 8)), jnp.float32)
    initial = normal_values(seeds[1], (SECTIONS, NODES), 0.3, 4.0, ((0, 4), (1, 8)), jnp.float32)
    capacitance = jnp.clip(jnp.exp(math.log(2.0) - 1.3862944 * jax.random.uniform(seeds[2], (SECTIONS, NODES), jnp.float32) ** shard_levels(seeds[2], (SECTIONS, NODES), ((0, 4), (1, 8)), -0.2, 0.2)), 0.5, 2.0)
    block_matrix = draw_block_matrix(jax.random.fold_in(seeds[10], 71), 0)
    block_inverse = draw_block_inverse(jax.random.fold_in(seeds[10], 71), 0)
    net_weight = normal_values(seeds[5], (SECTIONS, NODES, NET), NODES ** -0.5, 0.125, ((0, 4), (1, 8)), jnp.float32)
    tap_nodes = plant(jax.random.randint(seeds[6], (SECTIONS, BND), 0, NODES_DEV), jax.random.fold_in(seeds[6], 1), 0, NODES_DEV - 1).astype(jnp.int32)
    drive_nodes = plant(jax.random.randint(seeds[7], (SECTIONS, BND), 0, NODES_DEV), jax.random.fold_in(seeds[7], 1), 0, NODES_DEV - 1).astype(jnp.int32)
    drive_gain = jnp.clip(jnp.exp(math.log(2.0) - 1.3862944 * jax.random.uniform(seeds[8], (SECTIONS, BND), jnp.float32) ** shard_levels(seeds[8], (SECTIONS, BND), ((0, 4), (1, 8)), -0.2, 0.2)), 0.5, 2.0)
    attenuation = draw_attenuation(jax.random.fold_in(seeds[10], 71), 0)
    return dict(source=source, initial=initial, capacitance=capacitance, block_matrix=block_matrix, block_inverse=block_inverse, net_weight=net_weight, tap_nodes=tap_nodes, drive_nodes=drive_nodes, drive_gain=drive_gain, attenuation=attenuation)


HIGH = lax.Precision.HIGHEST

def reference(source, initial, capacitance, block_matrix, block_inverse, net_weight, tap_nodes, drive_nodes, drive_gain, attenuation):
    owner = jnp.arange(BND, dtype=jnp.int32) // BND_DEV * NODES_DEV
    tap_global = tap_nodes + owner[None, :]
    drive_global = drive_nodes + owner[None, :]
    waveform = jnp.broadcast_to(initial[:, None, :], (SECTIONS, STEPS, NODES)).astype(jnp.float32)
    cap_blocks = capacitance.reshape(SECTIONS, BLOCKS, BLOCK)
    history = []
    for sweep_index in range(SWEEPS):
        taps = jnp.take_along_axis(waveform, jnp.broadcast_to(tap_global[:, None, :], (SECTIONS, STEPS, BND)), axis=2)

        def relay(carried, pieces):
            decay, tapped = pieces
            return (decay[None, :] * carried + tapped, carried)
        zero_state = jnp.zeros((STEPS, BND), jnp.float32)
        unused, drive = lax.scan(relay, zero_state, (attenuation, taps))

        def place(values, gains, indices):
            return jnp.zeros((STEPS, NODES), jnp.float32).at[:, indices].add(values * gains[None, :])
        inject = jax.vmap(place)(drive, drive_gain, drive_global)
        for newton_index in range(NEWTON):
            net_volts = jnp.einsum('stn,snm->stm', waveform, net_weight, precision=HIGH)
            back = jnp.einsum('stm,snm->stn', net_volts, net_weight, precision=HIGH)
            previous = jnp.concatenate([initial[:, None, :], waveform[:, :-1, :]], axis=1)
            shaped = waveform.reshape(SECTIONS, STEPS, BLOCKS, BLOCK)
            applied = jnp.einsum('skij,stkj->stki', block_matrix, shaped, precision=HIGH).reshape(SECTIONS, STEPS, NODES)
            residual = applied - capacitance[:, None, :] * previous + 0.5 * jnp.tanh(waveform) + back - source - inject
            mean_sq = jnp.sum(residual * residual) / (SECTIONS * STEPS * NODES)
            damping = 1.0 / (1.0 + jnp.sqrt(mean_sq))
            res_blocks = residual.reshape(SECTIONS, STEPS, BLOCKS, BLOCK).transpose(1, 0, 2, 3)

            def march(carried, res_step):
                total = res_step + cap_blocks * carried
                fresh = jnp.einsum('skij,skj->ski', block_inverse, total, precision=HIGH)
                return (fresh, fresh)
            start = jnp.zeros((SECTIONS, BLOCKS, BLOCK), jnp.float32)
            unused_last, correction = lax.scan(march, start, res_blocks)
            correction = correction.transpose(1, 0, 2, 3).reshape(SECTIONS, STEPS, NODES)
            waveform = waveform - damping * correction
            history.append(mean_sq)
    return (waveform, jnp.stack(history))
```

```python
import functools

import jax
import jax.numpy as jnp
from jax import lax
from jax.experimental import pallas as pl
from jax.experimental.pallas import tpu as pltpu
from jax.sharding import PartitionSpec as P

NEWTON = 2
SWEEPS = 2
HIGHEST = lax.Precision.HIGHEST
F32 = jnp.float32
BF16 = jnp.bfloat16
LANES = 128
SUB = 8


def fdot(a, b):
    return jnp.dot(a, b, precision=HIGHEST, preferred_element_type=F32)


def bdot(a, b):
    return jnp.dot(a, b, preferred_element_type=F32)


def split(x):
    high = x.astype(BF16)
    return high, (x - high.astype(F32)).astype(BF16)


def dot3(x, high, low):
    rows = x.shape[0]
    xh, xl = split(x)
    both = bdot(jnp.concatenate([xh, xl], axis=0), high)
    return both[:rows] + both[rows:] + bdot(xh, low)


def dot2(x, exact):
    rows = x.shape[0]
    xh, xl = split(x)
    both = bdot(jnp.concatenate([xh, xl], axis=0), exact)
    return both[:rows] + both[rows:]


def lag(x, offset):
    if offset == 0:
        return x
    if offset >= x.shape[0]:
        return jnp.zeros_like(x)
    if offset % SUB == 0:
        return jnp.concatenate([jnp.zeros((offset, x.shape[1]), F32), x[: x.shape[0] - offset]], axis=0)
    row = lax.broadcasted_iota(jnp.int32, x.shape, 0)
    return jnp.where(row >= offset, pltpu.roll(x, offset, 0), 0.0)


def stages(steps):
    plan = [(0, 1)]
    span = 2
    while span < steps:
        wide = min(4, -(-steps // span))
        plan.append(tuple(span * i for i in range(1, wide)))
        span *= wide
    return plan


def powers_of(plan):
    return [p for stage in plan[1:] for p in stage]


def tile_sum(x):
    total = None
    for i in range(0, x.shape[0], SUB):
        for j in range(0, x.shape[1], LANES):
            part = x[i : i + SUB, j : j + LANES]
            total = part if total is None else total + part
    return total


def first_kernel(source, initial, capacitance, matrix, weight, tap, drive, gain, att, msg, pack):
    steps, nodes = source.shape
    blocks, width = matrix.shape[0], matrix.shape[1]
    channels = tap.shape[1]
    start = initial[...]
    net = fdot(start, weight[...])
    rows = []
    for j in range(0, net.shape[1], LANES):
        rows.append(net[:, j : j + LANES])
    node = lax.broadcasted_iota(jnp.int32, (nodes, channels), 0)
    taps = fdot(start, (node == tap[...]).astype(F32))
    for row in (taps, att[...]):
        for j in range(0, channels, LANES):
            rows.append(row[:, j : j + LANES])
    assert len(rows) <= SUB
    rows += [jnp.zeros((1, LANES), F32)] * (SUB - len(rows))
    tile = jnp.concatenate(rows, axis=0)
    msg[...] = jnp.broadcast_to(tile[None], msg.shape)
    pack[0:steps, :] = source[...]
    parts = []
    for k in range(blocks):
        parts.append(
            lax.dot_general(
                start[:, k * width : (k + 1) * width],
                matrix[k],
                (((1,), (1,)), ((), ())),
                precision=HIGHEST,
                preferred_element_type=F32,
            )
        )
    held = jnp.concatenate(parts, axis=1) - capacitance[...] * start
    pad = jnp.zeros((1, nodes - channels), F32)
    pack[steps : steps + SUB, :] = jnp.concatenate(
        [
            held,
            start,
            capacitance[...],
            jnp.concatenate([gain[...], pad], axis=1),
            jnp.concatenate([tap[...].astype(F32), pad], axis=1),
            jnp.concatenate([drive[...].astype(F32), pad], axis=1),
            jnp.zeros((2, nodes), F32),
        ],
        axis=0,
    )


def both(ref_other, ref_own, lo, hi):
    return jnp.concatenate([ref_other[lo:hi, :], ref_own[lo:hi, :]], axis=1)


def prep_kernel(plan, steps, channels, w_other, w_own, i_other, i_own, p_other, p_own, wh, wl, th, tl, ah, al, tap, drv):
    nodes = w_own.shape[0]
    blocks, width = i_own.shape[0], i_own.shape[1]
    cap = both(p_other, p_own, steps + 2, steps + 3)
    for half, ref in enumerate((w_other, w_own)):
        here = slice(half * nodes, (half + 1) * nodes)
        h, l = split(ref[...])
        wh[here, :] = h
        wl[here, :] = l
        turned = ref[...].T
        h, l = split(turned)
        th[:, here] = h
        tl[:, here] = l
    wanted = powers_of(plan)
    eye = lax.broadcasted_iota(jnp.int32, (width, width), 0) == lax.broadcasted_iota(jnp.int32, (width, width), 1)
    for b in range(2 * blocks):
        inverse = (i_other if b < blocks else i_own)[b % blocks].T
        scale = jnp.where(eye, cap[:, b * width : (b + 1) * width], 0.0)
        step = fdot(scale, inverse)
        made = {1: step}
        todo = [inverse, fdot(inverse, step)]
        power = 2
        while power <= max(wanted):
            made[power] = fdot(made[power // 2], made[power // 2])
            power *= 2
        for p in wanted:
            if p not in made:
                top = 1 << (p.bit_length() - 1)
                made[p] = fdot(made[top], made[p - top])
            todo.append(made[p])
        for i, value in enumerate(todo):
            h, l = split(value)
            ah[i, b] = h
            al[i, b] = l
    for half, ref in enumerate((p_other, p_own)):
        taps = ref[steps + 4 : steps + 5, 0:channels]
        node = lax.broadcasted_iota(jnp.int32, (nodes, channels), 0).astype(F32)
        tap[half] = (node == taps).astype(F32).astype(BF16)
        driven = ref[steps + 5 : steps + 6, 0:channels]
        drv[half] = (node == driven).astype(F32).T.astype(BF16)


def march(plan, r, ah, al):
    blocks, width = ah.shape[1], ah.shape[2]
    out = []
    for b in range(blocks):
        x = r[:, b * width : (b + 1) * width]
        unit = 0
        for s, stage in enumerate(plan):
            total = None
            for offset in stage:
                part = dot3(lag(x, offset), ah[unit, b], al[unit, b])
                total = part if total is None else total + part
                unit += 1
            x = total if s == 0 else total + x
        out.append(x)
    return jnp.concatenate(out, axis=1)


def finish_round(plan, r, c_ref, p_ref, msg, ah, al, wh, wl, north):
    tile = tile_sum(r * r) * north
    msg[...] = jnp.broadcast_to(tile[None], msg.shape)
    c = march(plan, r, ah, al)
    c_ref[...] = c
    p_ref[...] = dot3(c, wh[...], wl[...])
    return c


def bit_masks(my, sections, level):
    mine, other = [], []
    for s in range(sections):
        here = s >> level
        mine.append(here == (my >> level))
        other.append(here == ((my >> level) ^ 1))
    return mine, other


def opening_kernel(plan, steps, channels, sections, doms, levels, info, got, p_other, p_own, ah, al, wh, wl, th, tl, drv,
                   w_ref, q_ref, r_ref, c_ref, p_ref, msg, inj_ref, mix_ref):
    my, chip = info[0], info[1]
    north = info[2].astype(F32)
    nets = wh.shape[1]
    net_rows = nets // LANES
    tap_rows = channels // LANES
    mine = jnp.zeros((SUB, LANES), F32)
    base = my * doms
    for d in range(doms):
        mine = mine + got[base + d]
    net = jnp.concatenate([mine[i : i + 1, :] for i in range(net_rows)], axis=1)

    def channel_row(s, first):
        pieces = []
        for half in range(2):
            tile = got[s * doms + 2 * chip + half]
            pieces += [tile[first + i : first + i + 1, :] for i in range(tap_rows)]
        return jnp.concatenate(pieces, axis=1)

    decay, carried, drive = [], None, jnp.zeros((1, 2 * channels), F32)
    for s in range(sections):
        a = channel_row(s, net_rows + tap_rows)
        decay.append(a)
        if carried is not None:
            drive = jnp.where(my == s, carried, drive)
        tapped = channel_row(s, net_rows)
        carried = tapped if carried is None else a * carried + tapped
    one = jnp.ones((1, 2 * channels), F32)
    rows = []
    for level in range(levels):
        bit = (my >> level) & 1
        own_a, other_a, past_a = one, one, one
        for s in range(sections):
            here = s >> level
            own_a = jnp.where(here == (my >> level), own_a * decay[s], own_a)
            other_a = jnp.where(here == ((my >> level) ^ 1), other_a * decay[s], other_a)
            past_a = jnp.where((here == (my >> level)) & (s < my), past_a * decay[s], past_a)
        rows += [jnp.where(bit == 1, one, other_a), jnp.where(bit == 1, own_a, one), jnp.where(bit == 1, past_a, 0.0)]
    mix_ref[...] = jnp.concatenate(rows, axis=0)

    gain = jnp.concatenate([p_other[steps + 3 : steps + 4, 0:channels], p_own[steps + 3 : steps + 4, 0:channels]], axis=1)
    inj = spread(jnp.broadcast_to(drive * gain, (SUB, 2 * channels)), drv)[0:1]
    inj_ref[...] = inj
    back = dot3(jnp.broadcast_to(net, (SUB, nets)), th[...], tl[...])[0:1]
    start = both(p_other, p_own, steps + 1, steps + 2)
    held = both(p_other, p_own, steps, steps + 1)
    q = (held + back - inj) - both(p_other, p_own, 0, steps)
    r = q + 0.5 * jnp.tanh(start)
    w_ref[...] = jnp.broadcast_to(start, w_ref.shape)
    q_ref[...] = q
    r_ref[...] = r
    finish_round(plan, r, c_ref, p_ref, msg, ah, al, wh, wl, north)


def spread(drive, drv):
    channels = drv.shape[1]
    return jnp.concatenate([dot2(drive[:, h * channels : (h + 1) * channels], drv[h]) for h in range(2)], axis=1)


def damping_of(got, cells):
    total = got[0]
    for i in range(1, got.shape[0]):
        total = total + got[i]
    mean = jnp.sum(jnp.sum(total, axis=0, keepdims=True), axis=1, keepdims=True) / cells
    return mean, 1.0 / (1.0 + jnp.sqrt(mean))


def round_kernel(plan, steps, channels, cells, mode, *refs):
    refs = list(refs)
    take = lambda n: [refs.pop(0) for _ in range(n)]
    (info, got, own, recv, w0, q0, r0, c0, ah, al, wh, wl, th, tl) = take(14)
    if mode == "taps":
        (tap,) = take(1)
    if mode == "drive":
        pre, inj, p_other, p_own, drv = take(5)
    w_ref, q_ref, r_ref, c_ref, p_ref, msg, mean_ref = take(7)
    north = info[2].astype(F32)
    mean, damp = damping_of(got, cells)
    mean_ref[...] = jnp.broadcast_to(mean, mean_ref.shape)
    back = dot3(own[...] + recv[...], th[...], tl[...])
    w = w0[...] - damp * c0[...]
    q = q0[...] - damp * (r0[...] + back)
    if mode == "drive":
        drive = pre[0:steps, :] - damp * pre[steps : 2 * steps, :]
        gain = jnp.concatenate([p_other[steps + 3 : steps + 4, 0:channels], p_own[steps + 3 : steps + 4, 0:channels]], axis=1)
        q = q - (spread(drive * gain, drv) - inj[...])
    r = q + 0.5 * jnp.tanh(w)
    w_ref[...] = w
    q_ref[...] = q
    r_ref[...] = r
    if mode != "last":
        c = finish_round(plan, r, c_ref, p_ref, msg, ah, al, wh, wl, north)
    else:
        tile = tile_sum(r * r) * north
        msg[...] = jnp.broadcast_to(tile[None], msg.shape)
        c = march(plan, r, ah, al)
        c_ref[...] = c
        half = w.shape[1] // 2
        p_ref[0:steps, :] = w[:, 0:half]
        p_ref[steps : 2 * steps, :] = c[:, 0:half]
    if mode == "taps":
        (tt_ref,) = take(1)
        half = w.shape[1] // 2
        for h in range(2):
            here = slice(h * half, (h + 1) * half)
            both_taps = dot2(jnp.concatenate([w[:, here], c[:, here]], axis=0), tap[h])
            tt_ref[:, h * channels : (h + 1) * channels] = both_taps


def last_kernel(steps, cells, info, got, w, c, given, m1, m2, m3, out, means):
    mean, damp = damping_of(got, cells)
    half = out.shape[1]
    north = info[2] == 1
    w_here = jnp.where(north, w[:, half : 2 * half], given[0:steps, :])
    c_here = jnp.where(north, c[:, half : 2 * half], given[steps : 2 * steps, :])
    out[...] = w_here - damp * c_here
    lane = lax.broadcasted_iota(jnp.int32, (1, LANES), 1)
    row = jnp.where(lane == 0, m1[...], jnp.where(lane == 1, m2[...], jnp.where(lane == 2, m3[...], mean)))
    means[...] = row


def call(kernel, outs, *args, smem=()):
    specs = [
        pl.BlockSpec(memory_space=pltpu.SMEM if i in smem else pltpu.VMEM) for i in range(len(args))
    ]
    return pl.pallas_call(
        kernel,
        out_shape=[jax.ShapeDtypeStruct(s, d) for s, d in outs],
        in_specs=specs,
        out_specs=[pl.BlockSpec(memory_space=pltpu.VMEM) for _ in outs],
    )(*args)


def per_device(
    source,
    initial,
    capacitance,
    block_matrix,
    block_inverse,
    net_weight,
    tap_nodes,
    drive_nodes,
    drive_gain,
    attenuation,
):
    source = source[0]
    block_matrix = block_matrix[0]
    block_inverse = block_inverse[0]
    net_weight = net_weight[0]
    steps, nodes = source.shape
    blocks, width = block_matrix.shape[:2]
    nets = net_weight.shape[1]
    channels = tap_nodes.shape[1]
    sections, doms = lax.axis_size("section"), lax.axis_size("dom")
    devices = sections * doms
    everywhere = ("section", "dom")
    wide = 2 * nodes
    cells = float(devices * steps * nodes)
    plan = stages(steps)
    units = 2 + len(powers_of(plan))
    levels = max(1, (sections - 1).bit_length())

    def swap(x):
        return lax.ppermute(x, "dom", [(i, i ^ 1) for i in range(doms)])

    def pair(x, odd, even):
        links = []
        for s in range(sections):
            for d in range(doms):
                ps, pd = odd(s, d) if d % 2 else even(s, d)
                links.append((s * doms + d, ps * doms + pd))
        return lax.ppermute(x, everywhere, links)

    def along_dom(x, bit):
        return pair(x, lambda s, d: (s, d ^ (2 << bit)), lambda s, d: (s ^ 1, d))

    def along_section(x, bit):
        return pair(x, lambda s, d: (s ^ (1 << bit), d), lambda s, d: (s, d ^ 2))

    def gather(msg):
        return lax.all_to_all(msg, everywhere, 0, 0, tiled=False)

    place = lax.axis_index("dom")
    info = jnp.stack([lax.axis_index("section"), place // 2, place % 2]).astype(jnp.int32)

    w_other = swap(net_weight)
    i_other = swap(block_inverse)
    message = ((devices, SUB, LANES), F32)
    msg, pack = call(
        first_kernel,
        [message, ((steps + SUB, nodes), F32)],
        source, initial, capacitance, block_matrix, net_weight, tap_nodes, drive_nodes, drive_gain, attenuation,
    )
    got = gather(msg)
    p_other = swap(pack)
    wh, wl, th, tl, ah, al, tap, drv = call(
        functools.partial(prep_kernel, plan, steps, channels),
        [
            ((wide, nets), BF16), ((wide, nets), BF16), ((nets, wide), BF16), ((nets, wide), BF16),
            ((units, 2 * blocks, width, width), BF16), ((units, 2 * blocks, width, width), BF16),
            ((2, nodes, channels), BF16), ((2, channels, nodes), BF16),
        ],
        w_other, net_weight, i_other, block_inverse, p_other, pack,
    )
    state = [((steps, wide), F32)] * 4
    w, q, r, c, part, msg, inj, mix = call(
        functools.partial(opening_kernel, plan, steps, channels, sections, doms, levels),
        state + [((steps, nets), F32), message, ((1, wide), F32), ((3 * levels, 2 * channels), F32)],
        info, got, p_other, pack, ah, al, wh, wl, th, tl, drv,
        smem=(0,),
    )
    means = []
    taps = None
    bits = (doms // 2 - 1).bit_length()
    for index in range(1, NEWTON * SWEEPS):
        own = part
        recv = jnp.zeros_like(part) if bits == 0 else along_dom(own, 0)
        got = gather(msg)
        for bit in range(1, bits):
            own = own + recv
            recv = along_dom(own, bit)
        last = index == NEWTON * SWEEPS - 1
        boundary = index % NEWTON == 0
        before = index % NEWTON == NEWTON - 1 and not last
        mode = "last" if last else "drive" if boundary else "taps" if before else "plain"
        extra = []
        if mode == "taps":
            extra = [tap]
        if mode == "drive":
            prefix, total = jnp.zeros_like(taps), taps
            for level in range(levels):
                if sections == 1:
                    break
                got_taps = along_section(total, level)
                prefix = prefix + mix[3 * level + 2][None] * got_taps
                total = mix[3 * level][None] * total + mix[3 * level + 1][None] * got_taps
            extra = [prefix, inj, p_other, pack, drv]
        outs = state + [((2 * steps, nodes), F32) if last else ((steps, nets), F32), message, ((1, LANES), F32)]
        if mode == "taps":
            outs = outs + [((2 * steps, 2 * channels), F32)]
        result = call(
            functools.partial(round_kernel, plan, steps, channels, cells, mode),
            outs,
            info, got, own, recv, w, q, r, c, ah, al, wh, wl, th, tl, *extra,
            smem=(0,),
        )
        w, q, r, c, part, msg, mean = result[:7]
        means.append(mean)
        if mode == "taps":
            taps = result[7]
    got = gather(msg)
    given = swap(part)
    out, history = call(
        functools.partial(last_kernel, steps, cells),
        [((steps, nodes), F32), ((1, LANES), F32)],
        info, got, w, c, given, *means,
        smem=(0,),
    )
    return (out[None], history[0, : NEWTON * SWEEPS])


def solution(mesh):
    return jax.shard_map(
        per_device,
        mesh=mesh,
        in_specs=(
            P("section", None, "dom"),
            P("section", "dom"),
            P("section", "dom"),
            P("section", "dom", None, None),
            P("section", "dom", None, None),
            P("section", "dom", None),
            P("section", "dom"),
            P("section", "dom"),
            P("section", "dom"),
            P("section", "dom"),
        ),
        out_specs=(P("section", None, "dom"), P()),
        check_vma=False,
    )
```

```python
import functools

import jax
import jax.numpy as jnp
from jax import lax
from jax.experimental import pallas as pl
from jax.experimental.pallas import tpu as pltpu
from jax.sharding import PartitionSpec as P


NEWTON = 2
SWEEPS = 2
HIGHEST = lax.Precision.HIGHEST
F32 = jnp.float32
BF16 = jnp.bfloat16
LANES = 128
SUB = 8


def fdot(a, b):
    return jnp.dot(a, b, precision=HIGHEST, preferred_element_type=F32)


def dot6(a, b):
    return fdot(a, b)


def bdot(a, b):
    return jnp.dot(a, b, preferred_element_type=F32)


def tdot(a, b):
    return lax.dot_general(a, b, (((1,), (1,)), ((), ())), preferred_element_type=F32)


def split(x):
    high = x.astype(BF16)
    return high, (x - high.astype(F32)).astype(BF16)


def dot3(x, high, low):
    rows = x.shape[0]
    xh, xl = split(x)
    both = bdot(jnp.concatenate([xh, xl], axis=0), high)
    return both[:rows] + both[rows:] + bdot(xh, low)


def dot2(x, exact):
    rows = x.shape[0]
    xh, xl = split(x)
    both = bdot(jnp.concatenate([xh, xl], axis=0), exact)
    return both[:rows] + both[rows:]


def lag(x, offset):
    if offset == 0:
        return x
    if offset >= x.shape[0]:
        return jnp.zeros_like(x)
    if offset % SUB == 0:
        return jnp.concatenate([jnp.zeros((offset, x.shape[1]), F32), x[: x.shape[0] - offset]], axis=0)
    row = lax.broadcasted_iota(jnp.int32, x.shape, 0)
    return jnp.where(row >= offset, pltpu.roll(x, offset, 0), 0.0)


def stages(steps):
    plan = [(0, 1)]
    span = 2
    while span < steps:
        wide = 2
        plan.append(tuple(span * i for i in range(1, wide)))
        span *= wide
    return plan


def powers_of(plan):
    return [p for stage in plan[1:] for p in stage]


def tile_sum(x):
    total = None
    for i in range(0, x.shape[0], SUB):
        for j in range(0, x.shape[1], LANES):
            part = x[i : i + SUB, j : j + LANES]
            total = part if total is None else total + part
    return total


def first_kernel(source, initial, capacitance, matrix, weight, tap, drive, gain, att, msg, pack,
                 b_initial, b_capacitance, b_matrix, b_weight, b_tap, b_drive, b_gain, b_att, sems):
    steps, nodes = source.shape
    blocks, width = matrix.shape[0], matrix.shape[1]
    channels = tap.shape[1]
    moves = [(initial, b_initial), (weight, b_weight), (att, b_att), (tap, b_tap), (matrix, b_matrix),
             (capacitance, b_capacitance), (drive, b_drive), (gain, b_gain), (source, pack.at[0:steps, :])]
    copies = [pltpu.make_async_copy(src, dst, sems.at[i]) for i, (src, dst) in enumerate(moves)]
    for copy in copies:
        copy.start()
    pack[steps : steps + SUB, :] = jnp.zeros((SUB, nodes), F32)
    for copy in copies:
        copy.wait()
    start = b_initial[...]
    net = dot6(start, b_weight[...])
    rows = []
    for j in range(0, net.shape[1], LANES):
        rows.append(net[:, j : j + LANES])
    node = lax.broadcasted_iota(jnp.int32, (nodes, channels), 0)
    taps = fdot(start, (node == b_tap[...]).astype(F32))
    for row in (taps, b_att[...]):
        for j in range(0, channels, LANES):
            rows.append(row[:, j : j + LANES])
    assert len(rows) <= SUB
    rows += [jnp.zeros((1, LANES), F32)] * (SUB - len(rows))
    tile = jnp.concatenate(rows, axis=0)
    msg[...] = jnp.broadcast_to(tile[None], msg.shape)
    parts = []
    for k in range(blocks):
        parts.append(
            lax.dot_general(
                start[:, k * width : (k + 1) * width],
                b_matrix[k],
                (((1,), (1,)), ((), ())),
                precision=HIGHEST,
                preferred_element_type=F32,
            )
        )
    held = jnp.concatenate(parts, axis=1) - b_capacitance[...] * start
    for i, row in enumerate((held, start, b_capacitance[...])):
        pack[steps + i : steps + i + 1, :] = row
    for i, row in enumerate((b_gain[...], b_tap[...].astype(F32), b_drive[...].astype(F32))):
        pack[steps + 3 + i : steps + 4 + i, 0:channels] = row


def both(ref_other, ref_own, lo, hi):
    return jnp.concatenate([ref_other[lo:hi, :], ref_own[lo:hi, :]], axis=1)


def prep_kernel(plan, steps, w_other, w_own, i_other, i_own, p_other, p_own, th, tl, wh, wl, ah, al,
                b_w, b_i, s_wh, s_wl, sems):
    nodes = w_own.shape[0]
    blocks, width = i_own.shape[0], i_own.shape[1]
    moves = [(i_other, b_i.at[0]), (i_own, b_i.at[1]), (w_other, b_w.at[0]), (w_own, b_w.at[1])]
    copies = [pltpu.make_async_copy(src, dst, sems.at[i]) for i, (src, dst) in enumerate(moves)]
    for copy in copies:
        copy.start()
    cap = both(p_other, p_own, steps + 2, steps + 3)
    for copy in copies[2:]:
        copy.wait()
    for half in range(2):
        here = slice(half * nodes, (half + 1) * nodes)
        h, l = split(b_w[half])
        s_wh[here, :] = h
        s_wl[here, :] = l
    backs = [pltpu.make_async_copy(s_wh, wh, sems.at[4]), pltpu.make_async_copy(s_wl, wl, sems.at[5])]
    for copy in backs:
        copy.start()
    for copy in copies[:2]:
        copy.wait()
    wanted = powers_of(plan)
    eye = lax.broadcasted_iota(jnp.int32, (width, width), 0) == lax.broadcasted_iota(jnp.int32, (width, width), 1)

    def times(x, y):
        return bdot(x[0], y[0]) + bdot(x[1], y[0]) + bdot(x[0], y[1])

    every = range(2 * blocks)
    inverse = [split(b_i[b // blocks, b % blocks].T) for b in every]
    scale = [split(jnp.where(eye, cap[:, b * width : (b + 1) * width], 0.0)) for b in every]
    made = {1: [split(times(scale[b], inverse[b])) for b in every]}
    todo = [inverse, [split(times(inverse[b], made[1][b])) for b in every]]
    power = 2
    while power <= max(wanted):
        made[power] = [split(times(x, x)) for x in made[power // 2]]
        power *= 2
    for p in wanted:
        if p not in made:
            top = 1 << (p.bit_length() - 1)
            made[p] = [split(times(made[top][b], made[p - top][b])) for b in every]
        todo.append(made[p])
    for i, value in enumerate(todo):
        for b in every:
            ah[i, b], al[i, b] = value[b]
    for half in range(2):
        here = slice(half * nodes, (half + 1) * nodes)
        h, l = split(b_w[half].T)
        th[:, here] = h
        tl[:, here] = l
    for copy in backs:
        copy.wait()


def march(plan, r, ah, al):
    blocks, width = ah.shape[1], ah.shape[2]
    out = []
    for b in range(blocks):
        x = r[:, b * width : (b + 1) * width]
        unit = 0
        for s, stage in enumerate(plan):
            total = None
            for offset in stage:
                part = dot3(lag(x, offset), ah[unit, b], al[unit, b])
                total = part if total is None else total + part
                unit += 1
            x = total if s == 0 else total + x
        out.append(x)
    return jnp.concatenate(out, axis=1)


def fetch(wh, wl, b_wh, b_wl, sems):
    copies = [pltpu.make_async_copy(wh, b_wh, sems.at[0]), pltpu.make_async_copy(wl, b_wl, sems.at[1])]
    for copy in copies:
        copy.start()
    return copies


def send_squares(r, north, msg):
    row = jnp.sum(tile_sum(r * r), axis=0, keepdims=True) * north
    msg[...] = jnp.broadcast_to(row[None], msg.shape)


def finish_round(plan, r, c_ref, p_ref, msg, ah, al, copies, b_wh, b_wl, north):
    send_squares(r, north, msg)
    c = march(plan, r, ah, al)
    c_ref[...] = c
    for copy in copies:
        copy.wait()
    p_ref[...] = dot3(c, b_wh[...], b_wl[...])
    return c


def opening_kernel(plan, steps, channels, sections, doms, levels, info, got, p_other, p_own, ah, al, th, tl, wh, wl,
                   w_ref, q_ref, c_ref, p_ref, msg, aux_ref, b_wh, b_wl, sems):
    copies = fetch(wh, wl, b_wh, b_wl, sems)
    my, chip = info[0], info[1]
    north = info[2].astype(F32)
    nets = th.shape[0]
    net_rows = nets // LANES
    tap_rows = channels // LANES
    mine = jnp.zeros((SUB, LANES), F32)
    base = my * doms
    for d in range(doms):
        mine = mine + got[base + d]
    net = jnp.concatenate([mine[i : i + 1, :] for i in range(net_rows)], axis=1)

    def channel_row(s, first):
        pieces = []
        for half in range(2):
            tile = got[s * doms + 2 * chip + half]
            pieces += [tile[first + i : first + i + 1, :] for i in range(tap_rows)]
        return jnp.concatenate(pieces, axis=1)

    decay, carried, drive = [], None, jnp.zeros((1, 2 * channels), F32)
    for s in range(sections):
        a = channel_row(s, net_rows + tap_rows)
        decay.append(a)
        if carried is not None:
            drive = jnp.where(my == s, carried, drive)
        tapped = channel_row(s, net_rows)
        carried = tapped if carried is None else a * carried + tapped
    one = jnp.ones((1, 2 * channels), F32)
    rows = []
    for level in range(levels):
        bit = (my >> level) & 1
        own_a, other_a, past_a = one, one, one
        for s in range(sections):
            here = s >> level
            own_a = jnp.where(here == (my >> level), own_a * decay[s], own_a)
            other_a = jnp.where(here == ((my >> level) ^ 1), other_a * decay[s], other_a)
            past_a = jnp.where((here == (my >> level)) & (s < my), past_a * decay[s], past_a)
        rows += [jnp.where(bit == 1, one, other_a), jnp.where(bit == 1, own_a, one), jnp.where(bit == 1, past_a, 0.0)]
    nodes = p_own.shape[1]
    kept = [
        jnp.concatenate([p_other[i : i + 1, 0:channels], p_own[i : i + 1, 0:channels]], axis=1)
        for i in (steps + 3, steps + 4, steps + 5)
    ]
    inj = spread(jnp.broadcast_to(drive * kept[0], (SUB, 2 * channels)), kept[2], nodes)[0:1]
    aux_ref[...] = jnp.zeros_like(aux_ref)
    aux_ref[0:1, 0 : inj.shape[1]] = inj
    for i, row in enumerate(kept + rows):
        aux_ref[1 + i : 2 + i, 0 : 2 * channels] = row
    back = dot3(jnp.broadcast_to(net, (SUB, nets)), th[...], tl[...])[0:1]
    start = both(p_other, p_own, steps + 1, steps + 2)
    held = both(p_other, p_own, steps, steps + 1)
    q = (held + back - inj) - both(p_other, p_own, 0, steps)
    r = q + 0.5 * jnp.tanh(start)
    w_ref[...] = jnp.broadcast_to(start, w_ref.shape)
    q_ref[...] = q
    finish_round(plan, r, c_ref, p_ref, msg, ah, al, copies, b_wh, b_wl, north)


def chosen(index, nodes):
    node = lax.broadcasted_iota(jnp.int32, (nodes, index.shape[1]), 0).astype(F32)
    return (node == index).astype(BF16)


def spread(drive, index, nodes):
    rows = drive.shape[0]
    channels = drive.shape[1] // 2
    out = []
    for h in range(2):
        here = slice(h * channels, (h + 1) * channels)
        xh, xl = split(drive[:, here])
        two = tdot(jnp.concatenate([xh, xl], axis=0), chosen(index[:, here], nodes))
        out.append(two[:rows] + two[rows:])
    return jnp.concatenate(out, axis=1)


def damping_of(got, cells):
    total = got[0]
    for i in range(1, got.shape[0]):
        total = total + got[i]
    mean = jnp.sum(jnp.sum(total, axis=0, keepdims=True), axis=1, keepdims=True) / cells
    return mean, 1.0 / (1.0 + jnp.sqrt(mean))


def advance(got, own, recv, w0, q0, c0, th, tl, cells, mean_ref):
    mean, damp = damping_of(got, cells)
    mean_ref[...] = jnp.broadcast_to(mean, mean_ref.shape)
    back = dot3(own[...] + recv[...], th[...], tl[...])
    w = w0[...] - damp * c0[...]
    q = q0[...] - damp * (q0[...] + 0.5 * jnp.tanh(w0[...]) + back)
    return w, q, damp


def round_kernel(plan, steps, channels, cells, mode, *refs):
    refs = list(refs)
    take = lambda n: [refs.pop(0) for _ in range(n)]
    (info, got, own, recv, w0, q0, c0, ah, al, th, tl, wh, wl, aux) = take(14)
    if mode == "drive":
        (pre,) = take(1)
    w_ref, q_ref, c_ref, p_ref, msg, mean_ref = take(6)
    if mode == "taps":
        (tt_ref,) = take(1)
    b_wh, b_wl, sems = take(3)
    copies = fetch(wh, wl, b_wh, b_wl, sems)
    north = info[2].astype(F32)
    w, q, damp = advance(got, own, recv, w0, q0, c0, th, tl, cells, mean_ref)
    if mode == "drive":
        drive = pre[0:steps, :] - damp * pre[steps : 2 * steps, :]
        gain, _, driven = (aux[i : i + 1, 0 : 2 * channels] for i in (1, 2, 3))
        q = q - (spread(drive * gain, driven, w.shape[1] // 2) - aux[0:1, 0 : w.shape[1]])
    r = q + 0.5 * jnp.tanh(w)
    w_ref[...] = w
    q_ref[...] = q
    c = finish_round(plan, r, c_ref, p_ref, msg, ah, al, copies, b_wh, b_wl, north)
    if mode == "taps":
        half = w.shape[1] // 2
        for h in range(2):
            here = slice(h * half, (h + 1) * half)
            there = slice(h * channels, (h + 1) * channels)
            tapped = chosen(aux[2:3, there], half)
            tt_ref[:, there] = dot2(jnp.concatenate([w[:, here], c[:, here]], axis=0), tapped)


def residual_kernel(cells, info, got, own, recv, w0, q0, c0, th, tl, w_ref, r_ref, msg, mean_ref):
    w, q, _ = advance(got, own, recv, w0, q0, c0, th, tl, cells, mean_ref)
    r = q + 0.5 * jnp.tanh(w)
    w_ref[...] = w
    r_ref[...] = r
    send_squares(r, info[2].astype(F32), msg)


def correct_kernel(plan, w_in, r_in, ah, al, w_ref, c_ref, give):
    steps = r_in.shape[0]
    c = march(plan, r_in[...], ah, al)
    half = c.shape[1] // 2
    w = w_in[...]
    w_ref[...] = w[:, half:]
    c_ref[...] = c[:, half:]
    give[0:steps, :] = w[:, 0:half]
    give[steps : 2 * steps, :] = c[:, 0:half]


def last_kernel(steps, cells, info, got, w, c, given, m1, m2, m3, out, means):
    mean, damp = damping_of(got, cells)
    north = info[2] == 1
    w_here = jnp.where(north, w[...], given[0:steps, :])
    c_here = jnp.where(north, c[...], given[steps : 2 * steps, :])
    out[...] = w_here - damp * c_here
    lane = lax.broadcasted_iota(jnp.int32, (1, LANES), 1)
    row = jnp.where(lane == 0, m1[...], jnp.where(lane == 1, m2[...], jnp.where(lane == 2, m3[...], mean)))
    means[...] = row


def call(kernel, outs, *args, smem=(), hbm=(), hbm_outs=(), scratch=()):
    def place(i, far, scalar=()):
        return pl.BlockSpec(memory_space=pltpu.SMEM if i in scalar else pltpu.HBM if i in far else pltpu.VMEM)

    args = [pltpu.with_memory_space_constraint(x, pltpu.HBM) if i in hbm else x for i, x in enumerate(args)]
    return pl.pallas_call(
        kernel,
        out_shape=[pltpu.HBM(s, d) if i in hbm_outs else jax.ShapeDtypeStruct(s, d) for i, (s, d) in enumerate(outs)],
        in_specs=[place(i, hbm, smem) for i in range(len(args))],
        out_specs=[place(i, hbm_outs) for i in range(len(outs))],
        scratch_shapes=scratch,
        compiler_params=pltpu.CompilerParams(vmem_limit_bytes=16 << 20),
    )(*args)


def per_device(
    source,
    initial,
    capacitance,
    block_matrix,
    block_inverse,
    net_weight,
    tap_nodes,
    drive_nodes,
    drive_gain,
    attenuation,
):
    source = source[0]
    block_matrix = block_matrix[0]
    block_inverse = block_inverse[0]
    net_weight = net_weight[0]
    steps, nodes = source.shape
    blocks, width = block_matrix.shape[:2]
    nets = net_weight.shape[1]
    channels = tap_nodes.shape[1]
    sections, doms = lax.axis_size("section"), lax.axis_size("dom")
    devices = sections * doms
    everywhere = ("section", "dom")
    wide = 2 * nodes
    cells = float(devices * steps * nodes)
    plan = stages(steps)
    units = 2 + len(powers_of(plan))
    levels = max(1, (sections - 1).bit_length())

    def swap(x):
        return lax.ppermute(x, "dom", [(i, i ^ 1) for i in range(doms)])

    def pair(x, odd, even):
        links = []
        for s in range(sections):
            for d in range(doms):
                ps, pd = odd(s, d) if d % 2 else even(s, d)
                links.append((s * doms + d, ps * doms + pd))
        return lax.ppermute(x, everywhere, links)

    def along_dom(x, bit):
        return pair(x, lambda s, d: (s, d ^ (2 << bit)), lambda s, d: (s ^ 1, d))

    def along_section(x, bit):
        return pair(x, lambda s, d: (s ^ (1 << bit), d), lambda s, d: (s, d ^ 2))

    def gather(msg):
        return lax.all_to_all(msg, everywhere, 0, 0, tiled=False)

    place = lax.axis_index("dom")
    info = jnp.stack([lax.axis_index("section"), place // 2, place % 2]).astype(jnp.int32)

    w_other = swap(net_weight)
    i_other = swap(block_inverse)
    first_message = ((devices, SUB, LANES), F32)
    message = ((devices, 1, LANES), F32)
    row = lambda n, d=F32: pltpu.VMEM((1, n), d)
    msg, pack = call(
        first_kernel,
        [first_message, ((steps + SUB, nodes), F32)],
        source, initial, capacitance, block_matrix, net_weight, tap_nodes, drive_nodes, drive_gain, attenuation,
        hbm=range(9),
        scratch=[
            row(nodes), row(nodes), pltpu.VMEM(block_matrix.shape, F32), pltpu.VMEM(net_weight.shape, F32),
            row(channels, jnp.int32), row(channels, jnp.int32), row(channels), row(channels),
            pltpu.SemaphoreType.DMA((9,)),
        ],
    )
    got = gather(msg)
    p_other = swap(pack)
    cut = ((units, 2 * blocks, width, width), BF16)
    th, tl, wh, wl, ah, al = call(
        functools.partial(prep_kernel, plan, steps),
        [((nets, wide), BF16), ((nets, wide), BF16), ((wide, nets), BF16), ((wide, nets), BF16), cut, cut],
        w_other, net_weight, i_other, block_inverse, p_other, pack,
        hbm=range(4),
        hbm_outs=(2, 3),
        scratch=[
            pltpu.VMEM((2, nodes, nets), F32), pltpu.VMEM((2, blocks, width, width), F32),
            pltpu.VMEM((wide, nets), BF16), pltpu.VMEM((wide, nets), BF16), pltpu.SemaphoreType.DMA((6,)),
        ],
    )
    state = [((steps, wide), F32)] * 3
    aux_shape = (-(-(4 + 3 * levels) // SUB) * SUB, max(wide, 2 * channels))
    landing = [pltpu.VMEM((wide, nets), BF16), pltpu.VMEM((wide, nets), BF16), pltpu.SemaphoreType.DMA((2,))]
    w, q, c, part, msg, aux = call(
        functools.partial(opening_kernel, plan, steps, channels, sections, doms, levels),
        state + [((steps, nets), F32), message, (aux_shape, F32)],
        info, got, p_other, pack, ah, al, th, tl, wh, wl,
        smem=(0,),
        hbm=(8, 9),
        scratch=landing,
    )
    means = []
    taps = None
    bits = (doms // 2 - 1).bit_length()
    for index in range(1, NEWTON * SWEEPS):
        own = part
        recv = jnp.zeros_like(part) if bits == 0 else along_dom(own, 0)
        got = gather(msg)
        for bit in range(1, bits):
            own = own + recv
            recv = along_dom(own, bit)
        if index == NEWTON * SWEEPS - 1:
            break
        boundary = index % NEWTON == 0
        before = index % NEWTON == NEWTON - 1
        mode = "drive" if boundary else "taps" if before else "plain"
        extra = []
        if mode == "drive":
            prefix, total = jnp.zeros_like(taps), taps
            mix = aux[4 : 4 + 3 * levels, : 2 * channels]
            for level in range(levels):
                if sections == 1:
                    break
                got_taps = along_section(total, level)
                prefix = prefix + mix[3 * level + 2][None] * got_taps
                total = mix[3 * level][None] * total + mix[3 * level + 1][None] * got_taps
            extra = [prefix]
        outs = state + [((steps, nets), F32), message, ((1, LANES), F32)]
        if mode == "taps":
            outs = outs + [((2 * steps, 2 * channels), F32)]
        result = call(
            functools.partial(round_kernel, plan, steps, channels, cells, mode),
            outs,
            info, got, own, recv, w, q, c, ah, al, th, tl, wh, wl, aux, *extra,
            smem=(0,),
            hbm=(11, 12),
            scratch=landing,
        )
        w, q, c, part, msg, mean = result[:6]
        means.append(mean)
        if mode == "taps":
            taps = result[6]
    w, r, msg, mean = call(
        functools.partial(residual_kernel, cells),
        [((steps, wide), F32), ((steps, wide), F32), message, ((1, LANES), F32)],
        info, got, own, recv, w, q, c, th, tl,
        smem=(0,),
    )
    means.append(mean)
    got = gather(msg)
    w, c, give = call(
        functools.partial(correct_kernel, plan),
        [((steps, nodes), F32), ((steps, nodes), F32), ((2 * steps, nodes), F32)],
        w, r, ah, al,
    )
    given = swap(give)
    out, history = call(
        functools.partial(last_kernel, steps, cells),
        [((steps, nodes), F32), ((1, LANES), F32)],
        info, got, w, c, given, *means,
        smem=(0,),
    )
    return (out[None], history[0, : NEWTON * SWEEPS])


def solution(mesh):
    return jax.shard_map(
        per_device,
        mesh=mesh,
        in_specs=(
            P("section", None, "dom"),
            P("section", "dom"),
            P("section", "dom"),
            P("section", "dom", None, None),
            P("section", "dom", None, None),
            P("section", "dom", None),
            P("section", "dom"),
            P("section", "dom"),
            P("section", "dom"),
            P("section", "dom"),
        ),
        out_specs=(P("section", None, "dom"), P()),
        check_vma=False,
    )
```

```python
import functools

import jax
import jax.numpy as jnp
from jax import lax
from jax.experimental import pallas as pl
from jax.experimental.pallas import tpu as pltpu
from jax.sharding import PartitionSpec as P


NEWTON = 2
SWEEPS = 2
HIGHEST = lax.Precision.HIGHEST
F32 = jnp.float32
BF16 = jnp.bfloat16
LANES = 128
SUB = 8


def fdot(a, b):
    return jnp.dot(a, b, precision=HIGHEST, preferred_element_type=F32)


def bdot(a, b):
    return jnp.dot(a, b, preferred_element_type=F32)


def tdot(a, b):
    return lax.dot_general(a, b, (((1,), (1,)), ((), ())), preferred_element_type=F32)


def split(x):
    high = x.astype(BF16)
    return high, (x - high.astype(F32)).astype(BF16)


def dot3(x, high, low):
    rows = x.shape[0]
    xh, xl = split(x)
    both = bdot(jnp.concatenate([xh, xl], axis=0), high)
    return both[:rows] + both[rows:] + bdot(xh, low)


def dot2(x, exact):
    rows = x.shape[0]
    xh, xl = split(x)
    both = bdot(jnp.concatenate([xh, xl], axis=0), exact)
    return both[:rows] + both[rows:]


def lag(x, offset):
    if offset == 0:
        return x
    if offset >= x.shape[0]:
        return jnp.zeros_like(x)
    if offset % SUB == 0:
        return jnp.concatenate([jnp.zeros((offset, x.shape[1]), F32), x[: x.shape[0] - offset]], axis=0)
    row = lax.broadcasted_iota(jnp.int32, x.shape, 0)
    return jnp.where(row >= offset, pltpu.roll(x, offset, 0), 0.0)


def stages(steps):
    plan = [(0, 1)]
    span = 2
    while span < steps:
        wide = 2
        plan.append(tuple(span * i for i in range(1, wide)))
        span *= wide
    return plan


def powers_of(plan):
    return [p for stage in plan[1:] for p in stage]


def tree(parts):
    while len(parts) > 1:
        parts = [parts[i] + parts[i + 1] if i + 1 < len(parts) else parts[i] for i in range(0, len(parts), 2)]
    return parts[0]


def tile_sum(x):
    return tree([x[i : i + SUB, j : j + LANES] for i in range(0, x.shape[0], SUB) for j in range(0, x.shape[1], LANES)])


def land(moves, sems):
    copies = [pltpu.make_async_copy(src, dst, sems.at[i]) for i, (src, dst) in enumerate(moves)]
    for copy in copies:
        copy.start()
    return copies


def first_kernel(initial, weight, tap, att, msg, b_initial, b_weight, b_tap, b_att, sems):
    nodes = initial.shape[1]
    channels = tap.shape[1]
    for copy in land([(weight, b_weight), (initial, b_initial), (tap, b_tap), (att, b_att)], sems):
        copy.wait()
    start = b_initial[...]
    net = fdot(start, b_weight[...])
    rows = []
    for j in range(0, net.shape[1], LANES):
        rows.append(net[:, j : j + LANES])
    node = lax.broadcasted_iota(jnp.int32, (nodes, channels), 0)
    taps = fdot(start, (node == b_tap[...]).astype(F32))
    for row in (taps, b_att[...]):
        for j in range(0, channels, LANES):
            rows.append(row[:, j : j + LANES])
    assert len(rows) <= SUB
    rows += [jnp.zeros((1, LANES), F32)] * (SUB - len(rows))
    tile = jnp.concatenate(rows, axis=0)
    msg[...] = jnp.broadcast_to(tile[None], msg.shape)


def pack_kernel(source, initial, capacitance, matrix, tap, drive, gain, pack,
                b_initial, b_capacitance, b_matrix, b_tap, b_drive, b_gain, sems):
    steps, nodes = source.shape
    blocks, width = matrix.shape[0], matrix.shape[1]
    channels = tap.shape[1]
    copies = land(
        [(initial, b_initial), (matrix, b_matrix), (capacitance, b_capacitance), (tap, b_tap), (drive, b_drive),
         (gain, b_gain), (source, pack.at[0:steps, :])],
        sems,
    )
    pack[steps : steps + SUB, :] = jnp.zeros((SUB, nodes), F32)
    for copy in copies:
        copy.wait()
    start = b_initial[...]
    parts = []
    for k in range(blocks):
        parts.append(
            lax.dot_general(
                start[:, k * width : (k + 1) * width],
                b_matrix[k],
                (((1,), (1,)), ((), ())),
                precision=HIGHEST,
                preferred_element_type=F32,
            )
        )
    held = jnp.concatenate(parts, axis=1) - b_capacitance[...] * start
    for i, row in enumerate((held, start, b_capacitance[...])):
        pack[steps + i : steps + i + 1, :] = row
    for i, row in enumerate((b_gain[...], b_tap[...].astype(F32), b_drive[...].astype(F32))):
        pack[steps + 3 + i : steps + 4 + i, 0:channels] = row


def both(ref_other, ref_own, lo, hi):
    return jnp.concatenate([ref_other[lo:hi, :], ref_own[lo:hi, :]], axis=1)


def prep_kernel(plan, steps, i_other, w_other, w_own, i_own, p_other, p_own, th, tl, ah, al, wh, wl,
                b_w, b_i, s_wh, s_wl, sems):
    nodes = w_own.shape[0]
    blocks, width = i_own.shape[0], i_own.shape[1]
    copies = land([(i_own, b_i), (w_other, b_w.at[0]), (w_own, b_w.at[1])], sems)
    cap = both(p_other, p_own, steps + 2, steps + 3)
    for copy in copies[1:]:
        copy.wait()
    for half in range(2):
        here = slice(half * nodes, (half + 1) * nodes)
        h, l = split(b_w[half])
        s_wh[here, :] = h
        s_wl[here, :] = l
    backs = [pltpu.make_async_copy(s_wh, wh, sems.at[3]), pltpu.make_async_copy(s_wl, wl, sems.at[4])]
    for copy in backs:
        copy.start()
    copies[0].wait()
    wanted = powers_of(plan)
    eye = lax.broadcasted_iota(jnp.int32, (width, width), 0) == lax.broadcasted_iota(jnp.int32, (width, width), 1)

    def times(x, y):
        return bdot(x[0], y[0]) + bdot(x[1], y[0]) + bdot(x[0], y[1])

    every = range(2 * blocks)
    inverse = [split((i_other if b < blocks else b_i)[b % blocks].T) for b in every]
    scale = [split(jnp.where(eye, cap[:, b * width : (b + 1) * width], 0.0)) for b in every]
    made = {1: [split(times(scale[b], inverse[b])) for b in every]}
    todo = [inverse, [split(times(inverse[b], made[1][b])) for b in every]]
    power = 2
    while power <= max(wanted):
        made[power] = [split(times(x, x)) for x in made[power // 2]]
        power *= 2
    for p in wanted:
        if p not in made:
            top = 1 << (p.bit_length() - 1)
            made[p] = [split(times(made[top][b], made[p - top][b])) for b in every]
        todo.append(made[p])
    for i, value in enumerate(todo):
        for b in every:
            ah[i, b], al[i, b] = value[b]
    for half in range(2):
        here = slice(half * nodes, (half + 1) * nodes)
        h, l = split(b_w[half].T)
        th[:, here] = h
        tl[:, here] = l
    for copy in backs:
        copy.wait()


def march(plan, x, ah, al):
    blocks, width = ah.shape[1], ah.shape[2]
    rows = x.shape[0]
    unit = 0
    for s, stage in enumerate(plan):
        sums = [None] * blocks
        for offset in stage:
            xh, xl = split(lag(x, offset))
            pair = jnp.concatenate([xh, xl], axis=0)
            for b in range(blocks):
                here = slice(b * width, (b + 1) * width)
                two = bdot(pair[:, here], ah[unit, b])
                part = two[:rows] + two[rows:] + bdot(xh[:, here], al[unit, b])
                sums[b] = part if sums[b] is None else sums[b] + part
            unit += 1
        total = jnp.concatenate(sums, axis=1)
        x = total if s == 0 else total + x
    return x


def send_squares(r, spot, msg):
    row = jnp.sum(tile_sum(r * r), axis=0, keepdims=True) * spot[2:3, :]
    msg[...] = jnp.broadcast_to(row, msg.shape)


def finish_round(plan, r, spot, c_ref, p_ref, msg, ah, al, sent, copies, wh, wl):
    near_msg, sem = sent
    send_squares(r, spot, near_msg)
    leaving = pltpu.make_async_copy(near_msg, msg, sem.at[0])
    leaving.start()
    c = march(plan, r, ah, al)
    c_ref[...] = c
    for copy in copies:
        copy.wait()
    p_ref[...] = dot3(c, wh[...], wl[...])
    leaving.wait()
    return c


def opening_kernel(plan, steps, channels, sections, doms, levels, spot, got, p_other, p_own, ah, al, th, tl, wh, wl,
                   w_ref, q_ref, r_ref, c_ref, p_ref, msg, aux_ref, near_h, near_l, sems, *sent):
    copies = land([(wh, near_h), (wl, near_l)], sems)
    my, chip = spot[0:1, :], spot[1:2, :]
    nets = th.shape[0]
    net_rows = nets // LANES
    tap_rows = channels // LANES
    mine = jnp.zeros((SUB, LANES), F32)
    for t in range(sections):
        whole = tree([got[t * doms + d] for d in range(doms)])
        mine = jnp.where(my == float(t), whole, mine)
    net = jnp.concatenate([mine[i : i + 1, :] for i in range(net_rows)], axis=1)

    tiles = []
    for t in range(sections):
        halves = []
        for half in range(2):
            tile = got[t * doms + half]
            for z in range(1, doms // 2):
                tile = jnp.where(chip == float(z), got[t * doms + 2 * z + half], tile)
            halves.append(tile)
        tiles.append(halves)

    def channel_row(s, first):
        pieces = []
        for half in range(2):
            pieces += [tiles[s][half][first + i : first + i + 1, :] for i in range(tap_rows)]
        return jnp.concatenate(pieces, axis=1)

    lanes = 2 * channels // LANES
    here = jnp.concatenate([my] * lanes, axis=1).astype(jnp.int32)
    decay, carried, drive = [], None, jnp.zeros((1, 2 * channels), F32)
    for s in range(sections):
        a = channel_row(s, net_rows + tap_rows)
        decay.append(a)
        if carried is not None:
            drive = jnp.where(here == s, carried, drive)
        tapped = channel_row(s, net_rows)
        carried = tapped if carried is None else a * carried + tapped
    one = jnp.ones((1, 2 * channels), F32)
    rows = []
    for level in range(levels):
        bit = (here >> level) & 1
        own_a, other_a, past_a = one, one, one
        for s in range(sections):
            up = s >> level
            own_a = jnp.where((here >> level) == up, own_a * decay[s], own_a)
            other_a = jnp.where(((here >> level) ^ 1) == up, other_a * decay[s], other_a)
            past_a = jnp.where(((here >> level) == up) & (here > s), past_a * decay[s], past_a)
        rows += [jnp.where(bit == 1, one, other_a), jnp.where(bit == 1, own_a, one), jnp.where(bit == 1, past_a, 0.0)]
    nodes = p_own.shape[1]
    kept = [
        jnp.concatenate([p_other[i : i + 1, 0:channels], p_own[i : i + 1, 0:channels]], axis=1)
        for i in (steps + 3, steps + 4, steps + 5)
    ]
    inj = spread(jnp.broadcast_to(drive * kept[0], (SUB, 2 * channels)), kept[2], nodes)[0:1]
    aux_ref[...] = jnp.zeros_like(aux_ref)
    aux_ref[0:1, 0 : inj.shape[1]] = inj
    for i, row in enumerate(kept + rows):
        aux_ref[1 + i : 2 + i, 0 : 2 * channels] = row
    back = dot3(jnp.broadcast_to(net, (SUB, nets)), th[...], tl[...])[0:1]
    start = both(p_other, p_own, steps + 1, steps + 2)
    held = both(p_other, p_own, steps, steps + 1)
    q = (held + back - inj) - both(p_other, p_own, 0, steps)
    r = q + 0.5 * jnp.tanh(start)
    w_ref[...] = jnp.broadcast_to(start, w_ref.shape)
    q_ref[...] = q
    r_ref[...] = r
    finish_round(plan, r, spot, c_ref, p_ref, msg, ah, al, sent, copies, near_h, near_l)


def chosen(index, nodes):
    node = lax.broadcasted_iota(jnp.int32, (nodes, index.shape[1]), 0).astype(F32)
    return (node == index).astype(BF16)


def spread(drive, index, nodes):
    rows = drive.shape[0]
    channels = drive.shape[1] // 2
    out = []
    for h in range(2):
        here = slice(h * channels, (h + 1) * channels)
        xh, xl = split(drive[:, here])
        two = tdot(jnp.concatenate([xh, xl], axis=0), chosen(index[:, here], nodes))
        out.append(two[:rows] + two[rows:])
    return jnp.concatenate(out, axis=1)


def damping_of(got, cells):
    total = tile_sum(got[...])
    mean = jnp.sum(jnp.sum(total, axis=0, keepdims=True), axis=1, keepdims=True) / cells
    return mean, 1.0 / (1.0 + jnp.sqrt(mean))


def back_kernel(own, recv, r0, th, tl, u_ref):
    u_ref[...] = r0[...] + dot3(own[...] + recv[...], th[...], tl[...])


def advance(got, u, w0, q0, c0, cells, mean_ref):
    mean, damp = damping_of(got, cells)
    mean_ref[...] = jnp.broadcast_to(mean, mean_ref.shape)
    return w0[...] - damp * c0[...], q0[...] - damp * u[...], damp


def round_kernel(plan, steps, channels, cells, mode, *refs):
    refs = list(refs)
    take = lambda n: [refs.pop(0) for _ in range(n)]
    (spot, got, u, w0, q0, c0, ah, al, wh, wl, aux) = take(11)
    if mode == "drive":
        (pre,) = take(1)
    w_ref, q_ref, r_ref, c_ref, p_ref, msg, mean_ref = take(7)
    if mode == "taps":
        (tt_ref,) = take(1)
    near_h, near_l, sems, *sent = take(5)
    copies = land([(wh, near_h), (wl, near_l)], sems)
    w, q, damp = advance(got, u, w0, q0, c0, cells, mean_ref)
    if mode == "drive":
        drive = pre[0:steps, :] - damp * pre[steps : 2 * steps, :]
        gain, _, driven = (aux[i : i + 1, 0 : 2 * channels] for i in (1, 2, 3))
        q = q - (spread(drive * gain, driven, w.shape[1] // 2) - aux[0:1, 0 : w.shape[1]])
    r = q + 0.5 * jnp.tanh(w)
    w_ref[...] = w
    q_ref[...] = q
    r_ref[...] = r
    c = finish_round(plan, r, spot, c_ref, p_ref, msg, ah, al, sent, copies, near_h, near_l)
    if mode == "taps":
        half = w.shape[1] // 2
        for h in range(2):
            here = slice(h * half, (h + 1) * half)
            there = slice(h * channels, (h + 1) * channels)
            tapped = chosen(aux[2:3, there], half)
            tt_ref[:, there] = dot2(jnp.concatenate([w[:, here], c[:, here]], axis=0), tapped)


def residual_kernel(cells, spot, got, u, w0, q0, c0, w_ref, r_ref, msg, mean_ref):
    w, q, _ = advance(got, u, w0, q0, c0, cells, mean_ref)
    r = q + 0.5 * jnp.tanh(w)
    w_ref[...] = w
    r_ref[...] = r
    send_squares(r, spot, msg)


def correct_kernel(plan, w_in, r_in, ah, al, w_ref, c_ref, give):
    steps = r_in.shape[0]
    c = march(plan, r_in[...], ah, al)
    half = c.shape[1] // 2
    w = w_in[...]
    w_ref[...] = w[:, half:]
    c_ref[...] = c[:, half:]
    give[0:steps, :] = w[:, 0:half]
    give[steps : 2 * steps, :] = c[:, 0:half]


def last_kernel(steps, cells, spot, got, w, c, given, m1, m2, m3, out, means):
    mean, damp = damping_of(got, cells)
    north = jnp.concatenate([spot[2:3, :]] * (out.shape[1] // LANES), axis=1) == 1.0
    w_here = jnp.where(north, w[...], given[0:steps, :])
    c_here = jnp.where(north, c[...], given[steps : 2 * steps, :])
    out[...] = w_here - damp * c_here
    lane = lax.broadcasted_iota(jnp.int32, (1, LANES), 1)
    row = jnp.where(lane == 0, m1[...], jnp.where(lane == 1, m2[...], jnp.where(lane == 2, m3[...], mean)))
    means[...] = row[0, 0 : means.shape[0]]


def call(kernel, outs, *args, hbm=(), hbm_outs=(), scratch=()):
    def place(i, far):
        return pl.BlockSpec(memory_space=pltpu.HBM if i in far else pltpu.VMEM)

    args = [pltpu.with_memory_space_constraint(x, pltpu.HBM) if i in hbm else x for i, x in enumerate(args)]
    return pl.pallas_call(
        kernel,
        out_shape=[pltpu.HBM(s, d) if i in hbm_outs else jax.ShapeDtypeStruct(s, d) for i, (s, d) in enumerate(outs)],
        in_specs=[place(i, hbm) for i in range(len(args))],
        out_specs=[place(i, hbm_outs) for i in range(len(outs))],
        scratch_shapes=scratch,
        compiler_params=pltpu.CompilerParams(vmem_limit_bytes=16 << 20),
    )(*args)


def per_device(
    source,
    initial,
    capacitance,
    block_matrix,
    block_inverse,
    net_weight,
    tap_nodes,
    drive_nodes,
    drive_gain,
    attenuation,
):
    source = source[0]
    block_matrix = block_matrix[0]
    block_inverse = block_inverse[0]
    net_weight = net_weight[0]
    steps, nodes = source.shape
    blocks, width = block_matrix.shape[:2]
    nets = net_weight.shape[1]
    channels = tap_nodes.shape[1]
    sections, doms = lax.axis_size("section"), lax.axis_size("dom")
    devices = sections * doms
    everywhere = ("section", "dom")
    wide = 2 * nodes
    cells = float(devices * steps * nodes)
    plan = stages(steps)
    units = 2 + len(powers_of(plan))
    levels = max(1, (sections - 1).bit_length())

    def swap(x):
        return lax.ppermute(x, "dom", [(i, i ^ 1) for i in range(doms)])

    def pair(x, odd, even):
        links = []
        for s in range(sections):
            for d in range(doms):
                ps, pd = odd(s, d) if d % 2 else even(s, d)
                links.append((s * doms + d, ps * doms + pd))
        return lax.ppermute(x, everywhere, links)

    def along_dom(x, bit):
        return pair(x, lambda s, d: (s, d ^ (2 << bit)), lambda s, d: (s ^ 1, d))

    def along_section(x, bit):
        return pair(x, lambda s, d: (s ^ (1 << bit), d), lambda s, d: (s, d ^ 2))

    def gather(msg):
        spread_out = msg.reshape((devices, -1, LANES))
        return lax.all_to_all(spread_out, everywhere, 0, 0, tiled=False).reshape(msg.shape)

    core = lax.axis_index("dom")
    spot = jnp.stack([lax.axis_index("section"), core // 2, core % 2] + [core] * 5).astype(F32)
    spot = jnp.broadcast_to(spot[:, None], (SUB, LANES))
    w_other = swap(net_weight)
    i_other = swap(block_inverse)
    first_message = ((devices, SUB, LANES), F32)
    message = ((devices, LANES), F32)
    row = lambda n, d=F32: pltpu.VMEM((1, n), d)
    (msg,) = call(
        first_kernel,
        [first_message],
        initial, net_weight, tap_nodes, attenuation,
        hbm=range(4),
        scratch=[
            row(nodes), pltpu.VMEM(net_weight.shape, F32), row(channels, jnp.int32), row(channels),
            pltpu.SemaphoreType.DMA((4,)),
        ],
    )
    got = gather(msg)
    (pack,) = call(
        pack_kernel,
        [((steps + SUB, nodes), F32)],
        source, initial, capacitance, block_matrix, tap_nodes, drive_nodes, drive_gain,
        hbm=range(7),
        scratch=[
            row(nodes), row(nodes), pltpu.VMEM(block_matrix.shape, F32),
            row(channels, jnp.int32), row(channels, jnp.int32), row(channels), pltpu.SemaphoreType.DMA((7,)),
        ],
    )
    p_other = swap(pack)
    cut = ((units, 2 * blocks, width, width), BF16)
    up, down = ((nets, wide), BF16), ((wide, nets), BF16)
    th, tl, ah, al, wh, wl = call(
        functools.partial(prep_kernel, plan, steps),
        [up, up, cut, cut, down, down],
        i_other, w_other, net_weight, block_inverse, p_other, pack,
        hbm=range(1, 4),
        hbm_outs=(4, 5),
        scratch=[
            pltpu.VMEM((2, nodes, nets), F32), pltpu.VMEM((blocks, width, width), F32),
            pltpu.VMEM(*down), pltpu.VMEM(*down), pltpu.SemaphoreType.DMA((5,)),
        ],
    )
    state = [((steps, wide), F32)] * 4
    landing = [pltpu.VMEM(*down), pltpu.VMEM(*down), pltpu.SemaphoreType.DMA((2,))]
    landing = landing + [pltpu.VMEM(*message), pltpu.SemaphoreType.DMA((1,))]
    aux_shape = (-(-(4 + 3 * levels) // SUB) * SUB, max(wide, 2 * channels))
    w, q, r, c, part, msg, aux = call(
        functools.partial(opening_kernel, plan, steps, channels, sections, doms, levels),
        state + [((steps, nets), F32), message, (aux_shape, F32)],
        spot, got, p_other, pack, ah, al, th, tl, wh, wl,
        hbm=(8, 9),
        hbm_outs=(5,),
        scratch=landing,
    )
    means = []
    taps = None
    bits = (doms // 2 - 1).bit_length()
    for index in range(1, NEWTON * SWEEPS):
        own = part
        recv = jnp.zeros_like(part) if bits == 0 else along_dom(own, 0)
        got = gather(msg)
        for bit in range(1, bits):
            own = own + recv
            recv = along_dom(own, bit)
        last = index == NEWTON * SWEEPS - 1
        (u,) = call(back_kernel, [((steps, wide), F32)], own, recv, r, th, tl)
        if last:
            break
        boundary = index % NEWTON == 0
        before = index % NEWTON == NEWTON - 1
        mode = "drive" if boundary else "taps" if before else "plain"
        extra = []
        if mode == "drive":
            prefix, total = jnp.zeros_like(taps), taps
            mix = aux[4 : 4 + 3 * levels, : 2 * channels]
            for level in range(levels):
                if sections == 1:
                    break
                got_taps = along_section(total, level)
                prefix = prefix + mix[3 * level + 2][None] * got_taps
                total = mix[3 * level][None] * total + mix[3 * level + 1][None] * got_taps
            extra = [prefix]
        outs = state + [((steps, nets), F32), message, ((1, LANES), F32)]
        if mode == "taps":
            outs = outs + [((2 * steps, 2 * channels), F32)]
        result = call(
            functools.partial(round_kernel, plan, steps, channels, cells, mode),
            outs,
            spot, got, u, w, q, c, ah, al, wh, wl, aux, *extra,
            hbm=(8, 9),
            hbm_outs=(5,),
            scratch=landing,
        )
        w, q, r, c, part, msg, mean = result[:7]
        means.append(mean)
        if mode == "taps":
            taps = result[7]
    w, r, msg, mean = call(
        functools.partial(residual_kernel, cells),
        [((steps, wide), F32), ((steps, wide), F32), message, ((1, LANES), F32)],
        spot, got, u, w, q, c,
    )
    means.append(mean)
    got = gather(msg)
    w, c, give = call(
        functools.partial(correct_kernel, plan),
        [((steps, nodes), F32), ((steps, nodes), F32), ((2 * steps, nodes), F32)],
        w, r, ah, al,
    )
    given = swap(give)
    out, history = call(
        functools.partial(last_kernel, steps, cells),
        [((steps, nodes), F32), ((NEWTON * SWEEPS,), F32)],
        spot, got, w, c, given, *means,
    )
    return (out[None], history)


def solution(mesh):
    return jax.shard_map(
        per_device,
        mesh=mesh,
        in_specs=(
            P("section", None, "dom"),
            P("section", "dom"),
            P("section", "dom"),
            P("section", "dom", None, None),
            P("section", "dom", None, None),
            P("section", "dom", None),
            P("section", "dom"),
            P("section", "dom"),
            P("section", "dom"),
            P("section", "dom"),
        ),
        out_specs=(P("section", None, "dom"), P()),
        check_vma=False,
    )
```

```python
import functools

import jax
import jax.numpy as jnp
from jax import lax
from jax.experimental import pallas as pl
from jax.experimental.pallas import tpu as pltpu
from jax.sharding import PartitionSpec as P


NEWTON = 2
SWEEPS = 2
HIGHEST = lax.Precision.HIGHEST
F32 = jnp.float32
BF16 = jnp.bfloat16
LANES = 128
SUB = 8


def fdot(a, b):
    return jnp.dot(a, b, precision=HIGHEST, preferred_element_type=F32)


def bdot(a, b):
    return jnp.dot(a, b, preferred_element_type=F32)


def tdot(a, b):
    return lax.dot_general(a, b, (((1,), (1,)), ((), ())), preferred_element_type=F32)


def split(x):
    high = x.astype(BF16)
    return high, (x - high.astype(F32)).astype(BF16)


def dot3(x, high, low):
    rows = x.shape[0]
    xh, xl = split(x)
    both = bdot(jnp.concatenate([xh, xl], axis=0), high)
    return both[:rows] + both[rows:] + bdot(xh, low)


def dot2(x, exact):
    rows = x.shape[0]
    xh, xl = split(x)
    both = bdot(jnp.concatenate([xh, xl], axis=0), exact)
    return both[:rows] + both[rows:]


def lag(x, offset):
    if offset == 0:
        return x
    if offset >= x.shape[0]:
        return jnp.zeros_like(x)
    if offset % SUB == 0:
        return jnp.concatenate([jnp.zeros((offset, x.shape[1]), F32), x[: x.shape[0] - offset]], axis=0)
    row = lax.broadcasted_iota(jnp.int32, x.shape, 0)
    return jnp.where(row >= offset, pltpu.roll(x, offset, 0), 0.0)


def stages(steps):
    plan = [(0, 1)]
    span = 2
    while span < steps:
        wide = 2
        plan.append(tuple(span * i for i in range(1, wide)))
        span *= wide
    return plan


def powers_of(plan):
    return [p for stage in plan[1:] for p in stage]


def tree(parts):
    while len(parts) > 1:
        parts = [parts[i] + parts[i + 1] if i + 1 < len(parts) else parts[i] for i in range(0, len(parts), 2)]
    return parts[0]


def tile_sum(x):
    return tree([x[i : i + SUB, j : j + LANES] for i in range(0, x.shape[0], SUB) for j in range(0, x.shape[1], LANES)])


def land(moves, sems):
    copies = [pltpu.make_async_copy(src, dst, sems.at[i]) for i, (src, dst) in enumerate(moves)]
    for copy in copies:
        copy.start()
    return copies


def first_kernel(initial, weight, tap, att, msg, b_initial, b_weight, b_tap, b_att, sems):
    nodes = initial.shape[1]
    channels = tap.shape[1]
    for copy in land([(weight, b_weight), (initial, b_initial), (tap, b_tap), (att, b_att)], sems):
        copy.wait()
    start = b_initial[...]
    net = fdot(start, b_weight[...])
    rows = []
    for j in range(0, net.shape[1], LANES):
        rows.append(net[:, j : j + LANES])
    node = lax.broadcasted_iota(jnp.int32, (nodes, channels), 0)
    taps = fdot(start, (node == b_tap[...]).astype(F32))
    for row in (taps, b_att[...]):
        for j in range(0, channels, LANES):
            rows.append(row[:, j : j + LANES])
    assert len(rows) <= SUB
    rows += [jnp.zeros((1, LANES), F32)] * (SUB - len(rows))
    tile = jnp.concatenate(rows, axis=0)
    msg[...] = jnp.broadcast_to(tile[None], msg.shape)


def pack_kernel(source, initial, capacitance, matrix, tap, drive, gain, inverse, pack, near_inverse,
                b_initial, b_capacitance, b_matrix, b_tap, b_drive, b_gain, sems):
    steps, nodes = source.shape
    blocks, width = matrix.shape[0], matrix.shape[1]
    channels = tap.shape[1]
    copies = land(
        [(initial, b_initial), (matrix, b_matrix), (capacitance, b_capacitance), (tap, b_tap), (drive, b_drive),
         (gain, b_gain), (source, pack.at[0:steps, :]), (inverse, near_inverse)],
        sems,
    )
    pack[steps : steps + SUB, :] = jnp.zeros((SUB, nodes), F32)
    for copy in copies:
        copy.wait()
    start = b_initial[...]
    parts = []
    for k in range(blocks):
        parts.append(
            lax.dot_general(
                start[:, k * width : (k + 1) * width],
                b_matrix[k],
                (((1,), (1,)), ((), ())),
                precision=HIGHEST,
                preferred_element_type=F32,
            )
        )
    held = jnp.concatenate(parts, axis=1) - b_capacitance[...] * start
    for i, row in enumerate((held, start, b_capacitance[...])):
        pack[steps + i : steps + i + 1, :] = row
    for i, row in enumerate((b_gain[...], b_tap[...].astype(F32), b_drive[...].astype(F32))):
        pack[steps + 3 + i : steps + 4 + i, 0:channels] = row


def both(ref_other, ref_own, lo, hi):
    return jnp.concatenate([ref_other[lo:hi, :], ref_own[lo:hi, :]], axis=1)


def prep_kernel(plan, w_other, w_own, i_other, i_own, cap_other, cap_own, th, tl, ah, al, b_w, sems):
    nodes = w_own.shape[0]
    blocks, width = i_own.shape[0], i_own.shape[1]
    copies = land([(w_other, b_w.at[0]), (w_own, b_w.at[1])], sems)
    cap = jnp.concatenate([cap_other[...], cap_own[...]], axis=1)
    wanted = powers_of(plan)
    eye = lax.broadcasted_iota(jnp.int32, (width, width), 0) == lax.broadcasted_iota(jnp.int32, (width, width), 1)

    def times(x, y):
        return bdot(x[0], y[0]) + bdot(x[1], y[0]) + bdot(x[0], y[1])

    every = range(2 * blocks)
    inverse = [split((i_other if b < blocks else i_own)[b % blocks].T) for b in every]
    scale = [split(jnp.where(eye, cap[:, b * width : (b + 1) * width], 0.0)) for b in every]
    made = {1: [split(times(scale[b], inverse[b])) for b in every]}
    todo = [inverse, [split(times(inverse[b], made[1][b])) for b in every]]
    power = 2
    while power <= max(wanted):
        made[power] = [split(times(x, x)) for x in made[power // 2]]
        power *= 2
    for p in wanted:
        if p not in made:
            top = 1 << (p.bit_length() - 1)
            made[p] = [split(times(made[top][b], made[p - top][b])) for b in every]
        todo.append(made[p])
    for i, value in enumerate(todo):
        for b in every:
            ah[i, b], al[i, b] = value[b]
    for copy in copies:
        copy.wait()
    for half in range(2):
        here = slice(half * nodes, (half + 1) * nodes)
        h, l = split(b_w[half].T)
        th[:, here] = h
        tl[:, here] = l


def march(plan, x, ah, al):
    blocks, width = ah.shape[1], ah.shape[2]
    rows = x.shape[0]
    unit = 0
    for s, stage in enumerate(plan):
        sums = [None] * blocks
        for offset in stage:
            xh, xl = split(lag(x, offset))
            pair = jnp.concatenate([xh, xl], axis=0)
            for b in range(blocks):
                here = slice(b * width, (b + 1) * width)
                two = bdot(pair[:, here], ah[unit, b])
                part = two[:rows] + two[rows:] + bdot(xh[:, here], al[unit, b])
                sums[b] = part if sums[b] is None else sums[b] + part
            unit += 1
        total = jnp.concatenate(sums, axis=1)
        x = total if s == 0 else total + x
    return x


def send_squares(r, spot, msg):
    row = jnp.sum(tile_sum(r * r), axis=0, keepdims=True) * spot[2:3, :]
    msg[...] = jnp.broadcast_to(row, msg.shape)


def finish_round(plan, r, spot, c_ref, p_ref, msg, ah, al, sent, th, tl):
    near_msg, sem = sent
    send_squares(r, spot, near_msg)
    leaving = pltpu.make_async_copy(near_msg, msg, sem.at[0])
    leaving.start()
    c = march(plan, r, ah, al)
    c_ref[...] = c
    rows = c.shape[0]
    ch, cl = split(c)
    two = tdot(jnp.concatenate([ch, cl], axis=0), th[...])
    p_ref[...] = two[:rows] + two[rows:] + tdot(ch, tl[...])
    leaving.wait()
    return c


def opening_kernel(plan, steps, channels, sections, doms, levels, spot, got, p_other, p_own, ah, al, th, tl,
                   w_ref, q_ref, r_ref, c_ref, p_ref, msg, aux_ref, *sent):
    my, chip = spot[0:1, :], spot[1:2, :]
    nets = th.shape[0]
    net_rows = nets // LANES
    tap_rows = channels // LANES
    mine = jnp.zeros((SUB, LANES), F32)
    for t in range(sections):
        whole = tree([got[t * doms + d] for d in range(doms)])
        mine = jnp.where(my == float(t), whole, mine)
    net = jnp.concatenate([mine[i : i + 1, :] for i in range(net_rows)], axis=1)

    tiles = []
    for t in range(sections):
        halves = []
        for half in range(2):
            tile = got[t * doms + half]
            for z in range(1, doms // 2):
                tile = jnp.where(chip == float(z), got[t * doms + 2 * z + half], tile)
            halves.append(tile)
        tiles.append(halves)

    def channel_row(s, first):
        pieces = []
        for half in range(2):
            pieces += [tiles[s][half][first + i : first + i + 1, :] for i in range(tap_rows)]
        return jnp.concatenate(pieces, axis=1)

    lanes = 2 * channels // LANES
    here = jnp.concatenate([my] * lanes, axis=1).astype(jnp.int32)
    decay, carried, drive = [], None, jnp.zeros((1, 2 * channels), F32)
    for s in range(sections):
        a = channel_row(s, net_rows + tap_rows)
        decay.append(a)
        if carried is not None:
            drive = jnp.where(here == s, carried, drive)
        tapped = channel_row(s, net_rows)
        carried = tapped if carried is None else a * carried + tapped
    one = jnp.ones((1, 2 * channels), F32)
    rows = []
    for level in range(levels):
        bit = (here >> level) & 1
        own_a, other_a, past_a = one, one, one
        for s in range(sections):
            up = s >> level
            own_a = jnp.where((here >> level) == up, own_a * decay[s], own_a)
            other_a = jnp.where(((here >> level) ^ 1) == up, other_a * decay[s], other_a)
            past_a = jnp.where(((here >> level) == up) & (here > s), past_a * decay[s], past_a)
        rows += [jnp.where(bit == 1, one, other_a), jnp.where(bit == 1, own_a, one), jnp.where(bit == 1, past_a, 0.0)]
    nodes = p_own.shape[1]
    kept = [
        jnp.concatenate([p_other[i : i + 1, 0:channels], p_own[i : i + 1, 0:channels]], axis=1)
        for i in (steps + 3, steps + 4, steps + 5)
    ]
    inj = spread(jnp.broadcast_to(drive * kept[0], (SUB, 2 * channels)), kept[2], nodes)[0:1]
    aux_ref[...] = jnp.zeros_like(aux_ref)
    aux_ref[0:1, 0 : inj.shape[1]] = inj
    for i, row in enumerate(kept + rows):
        aux_ref[1 + i : 2 + i, 0 : 2 * channels] = row
    back = dot3(jnp.broadcast_to(net, (SUB, nets)), th[...], tl[...])[0:1]
    start = both(p_other, p_own, steps + 1, steps + 2)
    held = both(p_other, p_own, steps, steps + 1)
    q = (held + back - inj) - both(p_other, p_own, 0, steps)
    r = q + 0.5 * jnp.tanh(start)
    w_ref[...] = jnp.broadcast_to(start, w_ref.shape)
    q_ref[...] = q
    r_ref[...] = r
    finish_round(plan, r, spot, c_ref, p_ref, msg, ah, al, sent, th, tl)


def chosen(index, nodes):
    node = lax.broadcasted_iota(jnp.int32, (nodes, index.shape[1]), 0).astype(F32)
    return (node == index).astype(BF16)


def spread(drive, index, nodes):
    rows = drive.shape[0]
    channels = drive.shape[1] // 2
    out = []
    for h in range(2):
        here = slice(h * channels, (h + 1) * channels)
        xh, xl = split(drive[:, here])
        two = tdot(jnp.concatenate([xh, xl], axis=0), chosen(index[:, here], nodes))
        out.append(two[:rows] + two[rows:])
    return jnp.concatenate(out, axis=1)


def damping_of(got, cells):
    total = tile_sum(got[...])
    mean = jnp.sum(jnp.sum(total, axis=0, keepdims=True), axis=1, keepdims=True) / cells
    return mean, 1.0 / (1.0 + jnp.sqrt(mean))


def back_kernel(own, recv, r0, th, tl, u_ref):
    u_ref[...] = r0[...] + dot3(own[...] + recv[...], th[...], tl[...])


def advance(got, u, w0, q0, c0, cells, mean_ref):
    mean, damp = damping_of(got, cells)
    mean_ref[...] = jnp.broadcast_to(mean, mean_ref.shape)
    return w0[...] - damp * c0[...], q0[...] - damp * u[...], damp


def round_kernel(plan, steps, channels, cells, mode, *refs):
    refs = list(refs)
    take = lambda n: [refs.pop(0) for _ in range(n)]
    (spot, got, u, w0, q0, c0, ah, al, th, tl, aux) = take(11)
    if mode == "drive":
        (pre,) = take(1)
    w_ref, q_ref, r_ref, c_ref, p_ref, msg, mean_ref = take(7)
    if mode == "taps":
        (tt_ref,) = take(1)
    sent = take(2)
    w, q, damp = advance(got, u, w0, q0, c0, cells, mean_ref)
    if mode == "drive":
        drive = pre[0:steps, :] - damp * pre[steps : 2 * steps, :]
        gain, _, driven = (aux[i : i + 1, 0 : 2 * channels] for i in (1, 2, 3))
        q = q - (spread(drive * gain, driven, w.shape[1] // 2) - aux[0:1, 0 : w.shape[1]])
    r = q + 0.5 * jnp.tanh(w)
    w_ref[...] = w
    q_ref[...] = q
    r_ref[...] = r
    c = finish_round(plan, r, spot, c_ref, p_ref, msg, ah, al, sent, th, tl)
    if mode == "taps":
        half = w.shape[1] // 2
        for h in range(2):
            here = slice(h * half, (h + 1) * half)
            there = slice(h * channels, (h + 1) * channels)
            tapped = chosen(aux[2:3, there], half)
            tt_ref[:, there] = dot2(jnp.concatenate([w[:, here], c[:, here]], axis=0), tapped)


def residual_kernel(cells, spot, got, u, w0, q0, c0, w_ref, r_ref, msg, mean_ref):
    w, q, _ = advance(got, u, w0, q0, c0, cells, mean_ref)
    r = q + 0.5 * jnp.tanh(w)
    w_ref[...] = w
    r_ref[...] = r
    send_squares(r, spot, msg)


def correct_kernel(plan, w_in, r_in, ah, al, w_ref, c_ref, give):
    steps = r_in.shape[0]
    c = march(plan, r_in[...], ah, al)
    half = c.shape[1] // 2
    w = w_in[...]
    w_ref[...] = w[:, half:]
    c_ref[...] = c[:, half:]
    give[0:steps, :] = w[:, 0:half]
    give[steps : 2 * steps, :] = c[:, 0:half]


def last_kernel(steps, cells, spot, got, w, c, given, m1, m2, m3, out, means):
    mean, damp = damping_of(got, cells)
    north = jnp.concatenate([spot[2:3, :]] * (out.shape[1] // LANES), axis=1) == 1.0
    w_here = jnp.where(north, w[...], given[0:steps, :])
    c_here = jnp.where(north, c[...], given[steps : 2 * steps, :])
    out[...] = w_here - damp * c_here
    lane = lax.broadcasted_iota(jnp.int32, (1, LANES), 1)
    row = jnp.where(lane == 0, m1[...], jnp.where(lane == 1, m2[...], jnp.where(lane == 2, m3[...], mean)))
    means[...] = row[0, 0 : means.shape[0]]


def call(kernel, outs, *args, hbm=(), hbm_outs=(), scratch=()):
    def place(i, far):
        return pl.BlockSpec(memory_space=pltpu.HBM if i in far else pltpu.VMEM)

    args = [pltpu.with_memory_space_constraint(x, pltpu.HBM) if i in hbm else x for i, x in enumerate(args)]
    return pl.pallas_call(
        kernel,
        out_shape=[pltpu.HBM(s, d) if i in hbm_outs else jax.ShapeDtypeStruct(s, d) for i, (s, d) in enumerate(outs)],
        in_specs=[place(i, hbm) for i in range(len(args))],
        out_specs=[place(i, hbm_outs) for i in range(len(outs))],
        scratch_shapes=scratch,
        compiler_params=pltpu.CompilerParams(vmem_limit_bytes=16 << 20),
    )(*args)


def per_device(
    source,
    initial,
    capacitance,
    block_matrix,
    block_inverse,
    net_weight,
    tap_nodes,
    drive_nodes,
    drive_gain,
    attenuation,
):
    source = source[0]
    block_matrix = block_matrix[0]
    block_inverse = block_inverse[0]
    net_weight = net_weight[0]
    steps, nodes = source.shape
    blocks, width = block_matrix.shape[:2]
    nets = net_weight.shape[1]
    channels = tap_nodes.shape[1]
    sections, doms = lax.axis_size("section"), lax.axis_size("dom")
    devices = sections * doms
    everywhere = ("section", "dom")
    wide = 2 * nodes
    cells = float(devices * steps * nodes)
    plan = stages(steps)
    units = 2 + len(powers_of(plan))
    levels = max(1, (sections - 1).bit_length())

    def swap(x):
        return lax.ppermute(x, "dom", [(i, i ^ 1) for i in range(doms)])

    def pair(x, odd, even):
        links = []
        for s in range(sections):
            for d in range(doms):
                ps, pd = odd(s, d) if d % 2 else even(s, d)
                links.append((s * doms + d, ps * doms + pd))
        return lax.ppermute(x, everywhere, links)

    def along_dom(x, bit):
        return pair(x, lambda s, d: (s, d ^ (2 << bit)), lambda s, d: (s ^ 1, d))

    def along_section(x, bit):
        return pair(x, lambda s, d: (s ^ (1 << bit), d), lambda s, d: (s, d ^ 2))

    def gather(msg):
        spread_out = msg.reshape((devices, -1, LANES))
        return lax.all_to_all(spread_out, everywhere, 0, 0, tiled=False).reshape(msg.shape)

    core = lax.axis_index("dom")
    spot = jnp.stack([lax.axis_index("section"), core // 2, core % 2] + [core] * 5).astype(F32)
    spot = jnp.broadcast_to(spot[:, None], (SUB, LANES))
    w_other = swap(net_weight)
    i_other = swap(block_inverse)
    cap_other = swap(capacitance)
    first_message = ((devices, SUB, LANES), F32)
    message = ((devices, LANES), F32)
    row = lambda n, d=F32: pltpu.VMEM((1, n), d)
    (msg,) = call(
        first_kernel,
        [first_message],
        initial, net_weight, tap_nodes, attenuation,
        hbm=range(4),
        scratch=[
            row(nodes), pltpu.VMEM(net_weight.shape, F32), row(channels, jnp.int32), row(channels),
            pltpu.SemaphoreType.DMA((4,)),
        ],
    )
    got = gather(msg)
    pack, i_own = call(
        pack_kernel,
        [((steps + SUB, nodes), F32), (block_inverse.shape, F32)],
        source, initial, capacitance, block_matrix, tap_nodes, drive_nodes, drive_gain, block_inverse,
        hbm=range(8),
        scratch=[
            row(nodes), row(nodes), pltpu.VMEM(block_matrix.shape, F32),
            row(channels, jnp.int32), row(channels, jnp.int32), row(channels), pltpu.SemaphoreType.DMA((8,)),
        ],
    )
    p_other = swap(pack)
    cut = ((units, 2 * blocks, width, width), BF16)
    up = ((nets, wide), BF16)
    th, tl, ah, al = call(
        functools.partial(prep_kernel, plan),
        [up, up, cut, cut],
        w_other, net_weight, i_other, i_own, cap_other, capacitance,
        hbm=range(2),
        scratch=[
            pltpu.VMEM((2, nodes, nets), F32), pltpu.SemaphoreType.DMA((2,)),
        ],
    )
    state = [((steps, wide), F32)] * 4
    landing = [pltpu.VMEM(*message), pltpu.SemaphoreType.DMA((1,))]
    aux_shape = (-(-(4 + 3 * levels) // SUB) * SUB, max(wide, 2 * channels))
    w, q, r, c, part, msg, aux = call(
        functools.partial(opening_kernel, plan, steps, channels, sections, doms, levels),
        state + [((steps, nets), F32), message, (aux_shape, F32)],
        spot, got, p_other, pack, ah, al, th, tl,
        hbm_outs=(5,),
        scratch=landing,
    )
    means = []
    taps = None
    bits = (doms // 2 - 1).bit_length()
    for index in range(1, NEWTON * SWEEPS):
        own = part
        recv = jnp.zeros_like(part) if bits == 0 else along_dom(own, 0)
        got = gather(msg)
        for bit in range(1, bits):
            own = own + recv
            recv = along_dom(own, bit)
        last = index == NEWTON * SWEEPS - 1
        (u,) = call(back_kernel, [((steps, wide), F32)], own, recv, r, th, tl)
        if last:
            break
        boundary = index % NEWTON == 0
        before = index % NEWTON == NEWTON - 1
        mode = "drive" if boundary else "taps" if before else "plain"
        extra = []
        if mode == "drive":
            prefix, total = jnp.zeros_like(taps), taps
            mix = aux[4 : 4 + 3 * levels, : 2 * channels]
            for level in range(levels):
                if sections == 1:
                    break
                got_taps = along_section(total, level)
                prefix = prefix + mix[3 * level + 2][None] * got_taps
                total = mix[3 * level][None] * total + mix[3 * level + 1][None] * got_taps
            extra = [prefix]
        outs = state + [((steps, nets), F32), message, ((1, LANES), F32)]
        if mode == "taps":
            outs = outs + [((2 * steps, 2 * channels), F32)]
        result = call(
            functools.partial(round_kernel, plan, steps, channels, cells, mode),
            outs,
            spot, got, u, w, q, c, ah, al, th, tl, aux, *extra,
            hbm_outs=(5,),
            scratch=landing,
        )
        w, q, r, c, part, msg, mean = result[:7]
        means.append(mean)
        if mode == "taps":
            taps = result[7]
    w, r, msg, mean = call(
        functools.partial(residual_kernel, cells),
        [((steps, wide), F32), ((steps, wide), F32), message, ((1, LANES), F32)],
        spot, got, u, w, q, c,
    )
    means.append(mean)
    got = gather(msg)
    w, c, give = call(
        functools.partial(correct_kernel, plan),
        [((steps, nodes), F32), ((steps, nodes), F32), ((2 * steps, nodes), F32)],
        w, r, ah, al,
    )
    given = swap(give)
    out, history = call(
        functools.partial(last_kernel, steps, cells),
        [((steps, nodes), F32), ((NEWTON * SWEEPS,), F32)],
        spot, got, w, c, given, *means,
    )
    return (out[None], history)


def solution(mesh):
    return jax.shard_map(
        per_device,
        mesh=mesh,
        in_specs=(
            P("section", None, "dom"),
            P("section", "dom"),
            P("section", "dom"),
            P("section", "dom", None, None),
            P("section", "dom", None, None),
            P("section", "dom", None),
            P("section", "dom"),
            P("section", "dom"),
            P("section", "dom"),
            P("section", "dom"),
        ),
        out_specs=(P("section", None, "dom"), P()),
        check_vma=False,
    )
```

```python
import functools

import jax
import jax.numpy as jnp
from jax import lax
from jax.experimental import pallas as pl
from jax.experimental.pallas import tpu as pltpu
from jax.sharding import PartitionSpec as P


NEWTON = 2
SWEEPS = 2
HIGHEST = lax.Precision.HIGHEST
F32 = jnp.float32
BF16 = jnp.bfloat16
LANES = 128
SUB = 8


def fdot(a, b):
    return jnp.dot(a, b, precision=HIGHEST, preferred_element_type=F32)


def bdot(a, b):
    return jnp.dot(a, b, preferred_element_type=F32)


def tdot(a, b):
    return lax.dot_general(a, b, (((1,), (1,)), ((), ())), preferred_element_type=F32)


def split(x):
    high = x.astype(BF16)
    return high, (x - high.astype(F32)).astype(BF16)


def dot3(x, high, low):
    rows = x.shape[0]
    xh, xl = split(x)
    both = bdot(jnp.concatenate([xh, xl], axis=0), high)
    return both[:rows] + both[rows:] + bdot(xh, low)


def dot2(x, exact):
    rows = x.shape[0]
    xh, xl = split(x)
    both = bdot(jnp.concatenate([xh, xl], axis=0), exact)
    return both[:rows] + both[rows:]


def lag(x, offset):
    if offset == 0:
        return x
    if offset >= x.shape[0]:
        return jnp.zeros_like(x)
    if offset % SUB == 0:
        return jnp.concatenate([jnp.zeros((offset, x.shape[1]), F32), x[: x.shape[0] - offset]], axis=0)
    row = lax.broadcasted_iota(jnp.int32, x.shape, 0)
    return jnp.where(row >= offset, pltpu.roll(x, offset, 0), 0.0)


def stages(steps):
    plan = [(0, 1)]
    span = 2
    while span < steps:
        plan.append((span,))
        span *= 2
    return plan


def powers_of(plan):
    return [p for stage in plan[1:] for p in stage]


def tree(parts):
    while len(parts) > 1:
        parts = [parts[i] + parts[i + 1] if i + 1 < len(parts) else parts[i] for i in range(0, len(parts), 2)]
    return parts[0]


def tile_sum(x):
    return tree([x[i : i + SUB, j : j + LANES] for i in range(0, x.shape[0], SUB) for j in range(0, x.shape[1], LANES)])


def land(moves, sems):
    copies = [pltpu.make_async_copy(src, dst, sems.at[i]) for i, (src, dst) in enumerate(moves)]
    for copy in copies:
        copy.start()
    return copies


def first_kernel(initial, weight, tap, att, msg, b_initial, b_weight, b_tap, b_att, sems):
    nodes = initial.shape[1]
    channels = tap.shape[1]
    copies = land([(initial, b_initial), (tap, b_tap), (att, b_att), (weight, b_weight)], sems)
    for copy in copies[:3]:
        copy.wait()
    start = b_initial[...]
    node = lax.broadcasted_iota(jnp.int32, (nodes, channels), 0)
    taps = fdot(start, (node == b_tap[...]).astype(F32))
    copies[3].wait()
    net = fdot(start, b_weight[...])
    rows = []
    for j in range(0, net.shape[1], LANES):
        rows.append(net[:, j : j + LANES])
    for row in (taps, b_att[...]):
        for j in range(0, channels, LANES):
            rows.append(row[:, j : j + LANES])
    assert len(rows) <= SUB
    rows += [jnp.zeros((1, LANES), F32)] * (SUB - len(rows))
    tile = jnp.concatenate(rows, axis=0)
    msg[...] = jnp.broadcast_to(tile[None], msg.shape)


def pack_kernel(source, initial, capacitance, matrix, tap, drive, gain, inverse, pack, near_inverse,
                b_initial, b_capacitance, b_matrix, b_tap, b_drive, b_gain, sems):
    steps, nodes = source.shape
    blocks, width = matrix.shape[0], matrix.shape[1]
    channels = tap.shape[1]
    copies = land(
        [(initial, b_initial), (matrix, b_matrix), (capacitance, b_capacitance), (tap, b_tap), (drive, b_drive),
         (gain, b_gain), (source, pack.at[0:steps, :]), (inverse, near_inverse)],
        sems,
    )
    pack[steps : steps + SUB, :] = jnp.zeros((SUB, nodes), F32)
    for copy in copies:
        copy.wait()
    start = b_initial[...]
    parts = []
    for k in range(blocks):
        parts.append(
            lax.dot_general(
                start[:, k * width : (k + 1) * width],
                b_matrix[k],
                (((1,), (1,)), ((), ())),
                precision=HIGHEST,
                preferred_element_type=F32,
            )
        )
    held = jnp.concatenate(parts, axis=1) - b_capacitance[...] * start
    for i, row in enumerate((held, start, b_capacitance[...])):
        pack[steps + i : steps + i + 1, :] = row
    for i, row in enumerate((b_gain[...], b_tap[...].astype(F32), b_drive[...].astype(F32))):
        pack[steps + 3 + i : steps + 4 + i, 0:channels] = row


def both(ref_other, ref_own, lo, hi):
    return jnp.concatenate([ref_other[lo:hi, :], ref_own[lo:hi, :]], axis=1)


def prep_kernel(plan, w_other, w_own, i_other, i_own, cap_other, cap_own, th, tl, ah, al, b_w, sems):
    nodes = w_own.shape[0]
    blocks, width = i_own.shape[0], i_own.shape[1]
    copies = land([(w_other, b_w.at[0]), (w_own, b_w.at[1])], sems)
    cap = jnp.concatenate([cap_other[...], cap_own[...]], axis=1)
    wanted = powers_of(plan)
    eye = lax.broadcasted_iota(jnp.int32, (width, width), 0) == lax.broadcasted_iota(jnp.int32, (width, width), 1)

    def times(x, y):
        return bdot(x[0], y[0]) + bdot(x[1], y[0]) + bdot(x[0], y[1])

    every = range(2 * blocks)
    inverse = [split((i_other if b < blocks else i_own)[b % blocks].T) for b in every]
    scale = [split(jnp.where(eye, cap[:, b * width : (b + 1) * width], 0.0)) for b in every]
    made = {1: [split(times(scale[b], inverse[b])) for b in every]}
    todo = [inverse, [split(times(inverse[b], made[1][b])) for b in every]]
    power = 2
    while power <= max(wanted):
        made[power] = [split(times(x, x)) for x in made[power // 2]]
        power *= 2
    for p in wanted:
        if p not in made:
            top = 1 << (p.bit_length() - 1)
            made[p] = [split(times(made[top][b], made[p - top][b])) for b in every]
        todo.append(made[p])
    for i, value in enumerate(todo):
        for b in every:
            here = slice(i * width, (i + 1) * width)
            ah[b, here, :], al[b, here, :] = value[b]
    for copy in copies:
        copy.wait()
    for half in range(2):
        here = slice(half * nodes, (half + 1) * nodes)
        h, l = split(b_w[half].T)
        th[:, here] = h
        tl[:, here] = l


def march(plan, x, ah, al):
    blocks, width = ah.shape[0], ah.shape[2]
    rows = x.shape[0]
    unit = 0
    for s, stage in enumerate(plan):
        parts = [split(lag(x, offset)) for offset in stage]
        there = slice(unit * width, (unit + len(stage)) * width)
        unit += len(stage)
        sums = []
        for b in range(blocks):
            here = slice(b * width, (b + 1) * width)
            xh = jnp.concatenate([h[:, here] for h, _ in parts], axis=1)
            xl = jnp.concatenate([l[:, here] for _, l in parts], axis=1)
            two = bdot(jnp.concatenate([xh, xl], axis=0), ah[b, there, :])
            sums.append(two[:rows] + two[rows:] + bdot(xh, al[b, there, :]))
        total = jnp.concatenate(sums, axis=1)
        x = total if s == 0 else total + x
    return x


def send_squares(r, spot, msg):
    row = jnp.sum(tile_sum(r * r), axis=0, keepdims=True) * spot[2:3, :]
    msg[...] = jnp.broadcast_to(row, msg.shape)


def finish_round(plan, r, spot, r_ref, c_ref, p_ref, msg, ah, al, sent, th, tl, more=None):
    near_msg, sem = sent
    r_ref[...] = r
    send_squares(r, spot, near_msg)
    leaving = pltpu.make_async_copy(near_msg, msg, sem.at[0])
    leaving.start()
    owner = jnp.max(spot[2:3, :]) > 0.5

    @pl.when(owner)
    def _():
        c = march(plan, r_ref[...], ah, al)
        c_ref[...] = c
        rows = c.shape[0]
        ch, cl = split(c)
        two = tdot(jnp.concatenate([ch, cl], axis=0), th[...])
        p_ref[...] = two[:rows] + two[rows:] + tdot(ch, tl[...])
        if more is not None:
            more(c)

    @pl.when(jnp.logical_not(owner))
    def _():
        c_ref[...] = jnp.zeros_like(c_ref)
        p_ref[...] = jnp.zeros_like(p_ref)

    leaving.wait()


def opening_kernel(plan, steps, channels, sections, doms, levels, spot, got, p_other, p_own, ah, al, th, tl,
                   w_ref, r_ref, c_ref, p_ref, msg, aux_ref, *sent):
    my, chip = spot[0:1, :], spot[1:2, :]
    nets = th.shape[0]
    net_rows = nets // LANES
    tap_rows = channels // LANES
    mine = jnp.zeros((SUB, LANES), F32)
    for t in range(sections):
        whole = tree([got[t * doms + d] for d in range(doms)])
        mine = jnp.where(my == float(t), whole, mine)
    net = jnp.concatenate([mine[i : i + 1, :] for i in range(net_rows)], axis=1)

    tiles = []
    for t in range(sections):
        halves = []
        for half in range(2):
            tile = got[t * doms + half]
            for z in range(1, doms // 2):
                tile = jnp.where(chip == float(z), got[t * doms + 2 * z + half], tile)
            halves.append(tile)
        tiles.append(halves)

    def channel_row(s, first):
        pieces = []
        for half in range(2):
            pieces += [tiles[s][half][first + i : first + i + 1, :] for i in range(tap_rows)]
        return jnp.concatenate(pieces, axis=1)

    lanes = 2 * channels // LANES
    here = jnp.concatenate([my] * lanes, axis=1).astype(jnp.int32)
    decay, carried, drive = [], None, jnp.zeros((1, 2 * channels), F32)
    for s in range(sections):
        a = channel_row(s, net_rows + tap_rows)
        decay.append(a)
        if carried is not None:
            drive = jnp.where(here == s, carried, drive)
        tapped = channel_row(s, net_rows)
        carried = tapped if carried is None else a * carried + tapped
    one = jnp.ones((1, 2 * channels), F32)
    rows = []
    for level in range(levels):
        bit = (here >> level) & 1
        own_a, other_a, past_a = one, one, one
        for s in range(sections):
            up = s >> level
            own_a = jnp.where((here >> level) == up, own_a * decay[s], own_a)
            other_a = jnp.where(((here >> level) ^ 1) == up, other_a * decay[s], other_a)
            past_a = jnp.where(((here >> level) == up) & (here > s), past_a * decay[s], past_a)
        rows += [jnp.where(bit == 1, one, other_a), jnp.where(bit == 1, own_a, one), jnp.where(bit == 1, past_a, 0.0)]
    nodes = p_own.shape[1]
    kept = [
        jnp.concatenate([p_other[i : i + 1, 0:channels], p_own[i : i + 1, 0:channels]], axis=1)
        for i in (steps + 3, steps + 4, steps + 5)
    ]
    inj = spread(jnp.broadcast_to(drive * kept[0], (SUB, 2 * channels)), kept[2], nodes)[0:1]
    aux_ref[...] = jnp.zeros_like(aux_ref)
    aux_ref[0:1, 0 : inj.shape[1]] = inj
    for i, row in enumerate(kept + rows):
        aux_ref[1 + i : 2 + i, 0 : 2 * channels] = row
    back = dot3(jnp.broadcast_to(net, (SUB, nets)), th[...], tl[...])[0:1]
    start = both(p_other, p_own, steps + 1, steps + 2)
    held = both(p_other, p_own, steps, steps + 1)
    q = (held + back - inj) - both(p_other, p_own, 0, steps)
    r = q + 0.5 * jnp.tanh(start)
    w_ref[...] = jnp.broadcast_to(start, w_ref.shape)
    finish_round(plan, r, spot, r_ref, c_ref, p_ref, msg, ah, al, sent, th, tl)


def chosen(index, nodes):
    node = lax.broadcasted_iota(jnp.int32, (nodes, index.shape[1]), 0).astype(F32)
    return (node == index).astype(BF16)


def spread(drive, index, nodes):
    rows = drive.shape[0]
    channels = drive.shape[1] // 2
    out = []
    for h in range(2):
        here = slice(h * channels, (h + 1) * channels)
        xh, xl = split(drive[:, here])
        two = tdot(jnp.concatenate([xh, xl], axis=0), chosen(index[:, here], nodes))
        out.append(two[:rows] + two[rows:])
    return jnp.concatenate(out, axis=1)


def damping_of(got, cells):
    total = tile_sum(got[...])
    mean = jnp.sum(jnp.sum(total, axis=0, keepdims=True), axis=1, keepdims=True) / cells
    return mean, 1.0 / (1.0 + jnp.sqrt(mean))


def back_kernel(own, recv, r0, th, tl, u_ref):
    u_ref[...] = r0[...] + dot3(own[...] + recv[...], th[...], tl[...])


def advance(got, u, w0, r0, c0, cells, mean_ref):
    mean, damp = damping_of(got, cells)
    mean_ref[...] = jnp.broadcast_to(mean, mean_ref.shape)
    q0 = r0[...] - 0.5 * jnp.tanh(w0[...])
    return w0[...] - damp * c0[...], q0 - damp * u[...], damp


def round_kernel(plan, steps, channels, cells, mode, *refs):
    refs = list(refs)
    take = lambda n: [refs.pop(0) for _ in range(n)]
    (spot, got, u, w0, r0, c0, ah, al, th, tl, aux) = take(11)
    if mode == "drive":
        (pre,) = take(1)
    w_ref, r_ref, c_ref, p_ref, msg, mean_ref = take(6)
    if mode == "taps":
        (tt_ref,) = take(1)
    sent = take(2)
    w, q, damp = advance(got, u, w0, r0, c0, cells, mean_ref)
    if mode == "drive":
        drive = pre[0:steps, :] - damp * pre[steps : 2 * steps, :]
        gain, _, driven = (aux[i : i + 1, 0 : 2 * channels] for i in (1, 2, 3))
        q = q - (spread(drive * gain, driven, w.shape[1] // 2) - aux[0:1, 0 : w.shape[1]])
    r = q + 0.5 * jnp.tanh(w)
    w_ref[...] = w
    half = w.shape[1] // 2

    def tap(c):
        for h in range(2):
            here = slice(h * half, (h + 1) * half)
            there = slice(h * channels, (h + 1) * channels)
            tapped = chosen(aux[2:3, there], half)
            tt_ref[:, there] = dot2(jnp.concatenate([w_ref[:, here], c[:, here]], axis=0), tapped)

    more = None
    if mode == "taps":
        more = tap
        tt_ref[...] = jnp.zeros_like(tt_ref)
    finish_round(plan, r, spot, r_ref, c_ref, p_ref, msg, ah, al, sent, th, tl, more)


def residual_kernel(cells, spot, got, u, w0, r0, c0, w_ref, r_ref, msg, mean_ref):
    w, q, _ = advance(got, u, w0, r0, c0, cells, mean_ref)
    r = q + 0.5 * jnp.tanh(w)
    w_ref[...] = w
    r_ref[...] = r
    send_squares(r, spot, msg)


def correct_kernel(plan, w_in, r_in, ah, al, w_ref, c_ref, give):
    steps = r_in.shape[0]
    c = march(plan, r_in[...], ah, al)
    half = c.shape[1] // 2
    w = w_in[...]
    w_ref[...] = w[:, half:]
    c_ref[...] = c[:, half:]
    give[0:steps, :] = w[:, 0:half]
    give[steps : 2 * steps, :] = c[:, 0:half]


def last_kernel(steps, cells, spot, got, w, c, given, m1, m2, m3, out, means):
    mean, damp = damping_of(got, cells)
    north = jnp.concatenate([spot[2:3, :]] * (out.shape[1] // LANES), axis=1) == 1.0
    w_here = jnp.where(north, w[...], given[0:steps, :])
    c_here = jnp.where(north, c[...], given[steps : 2 * steps, :])
    out[...] = w_here - damp * c_here
    lane = lax.broadcasted_iota(jnp.int32, (1, LANES), 1)
    row = jnp.where(lane == 0, m1[...], jnp.where(lane == 1, m2[...], jnp.where(lane == 2, m3[...], mean)))
    means[...] = row[0, 0 : means.shape[0]]


def call(kernel, outs, *args, hbm=(), hbm_outs=(), scratch=()):
    def place(i, far):
        return pl.BlockSpec(memory_space=pltpu.HBM if i in far else pltpu.VMEM)

    args = [pltpu.with_memory_space_constraint(x, pltpu.HBM) if i in hbm else x for i, x in enumerate(args)]
    return pl.pallas_call(
        kernel,
        out_shape=[pltpu.HBM(s, d) if i in hbm_outs else jax.ShapeDtypeStruct(s, d) for i, (s, d) in enumerate(outs)],
        in_specs=[place(i, hbm) for i in range(len(args))],
        out_specs=[place(i, hbm_outs) for i in range(len(outs))],
        scratch_shapes=scratch,
        compiler_params=pltpu.CompilerParams(vmem_limit_bytes=16 << 20),
    )(*args)


def per_device(
    source,
    initial,
    capacitance,
    block_matrix,
    block_inverse,
    net_weight,
    tap_nodes,
    drive_nodes,
    drive_gain,
    attenuation,
):
    source = source[0]
    block_matrix = block_matrix[0]
    block_inverse = block_inverse[0]
    net_weight = net_weight[0]
    steps, nodes = source.shape
    blocks, width = block_matrix.shape[:2]
    nets = net_weight.shape[1]
    channels = tap_nodes.shape[1]
    sections, doms = lax.axis_size("section"), lax.axis_size("dom")
    devices = sections * doms
    everywhere = ("section", "dom")
    wide = 2 * nodes
    cells = float(devices * steps * nodes)
    plan = stages(steps)
    units = 2 + len(powers_of(plan))
    levels = max(1, (sections - 1).bit_length())

    def swap(x):
        return lax.ppermute(x, "dom", [(i, i ^ 1) for i in range(doms)])

    def pair(x, odd, even):
        links = []
        for s in range(sections):
            for d in range(doms):
                ps, pd = odd(s, d) if d % 2 else even(s, d)
                links.append((s * doms + d, ps * doms + pd))
        return lax.ppermute(x, everywhere, links)

    def along_dom(x, bit):
        return pair(x, lambda s, d: (s, d ^ (2 << bit)), lambda s, d: (s ^ 1, d))

    def along_section(x, bit):
        return pair(x, lambda s, d: (s ^ (1 << bit), d), lambda s, d: (s, d ^ 2))

    def gather(msg):
        spread_out = msg.reshape((devices, -1, LANES))
        return lax.all_to_all(spread_out, everywhere, 0, 0, tiled=False).reshape(msg.shape)

    core = lax.axis_index("dom")
    spot = jnp.stack([lax.axis_index("section"), core // 2, core % 2] + [core] * 5).astype(F32)
    spot = jnp.broadcast_to(spot[:, None], (SUB, LANES))
    w_other = swap(net_weight)
    i_other = swap(block_inverse)
    cap_other = swap(capacitance)
    first_message = ((devices, SUB, LANES), F32)
    message = ((devices, LANES), F32)
    row = lambda n, d=F32: pltpu.VMEM((1, n), d)
    (msg,) = call(
        first_kernel,
        [first_message],
        initial, net_weight, tap_nodes, attenuation,
        hbm=range(4),
        scratch=[
            row(nodes), pltpu.VMEM(net_weight.shape, F32), row(channels, jnp.int32), row(channels),
            pltpu.SemaphoreType.DMA((4,)),
        ],
    )
    got = gather(msg)
    pack, i_own = call(
        pack_kernel,
        [((steps + SUB, nodes), F32), (block_inverse.shape, F32)],
        source, initial, capacitance, block_matrix, tap_nodes, drive_nodes, drive_gain, block_inverse,
        hbm=range(8),
        scratch=[
            row(nodes), row(nodes), pltpu.VMEM(block_matrix.shape, F32),
            row(channels, jnp.int32), row(channels, jnp.int32), row(channels), pltpu.SemaphoreType.DMA((8,)),
        ],
    )
    p_other = swap(pack)
    cut = ((2 * blocks, units * width, width), BF16)
    up = ((nets, wide), BF16)
    th, tl, ah, al = call(
        functools.partial(prep_kernel, plan),
        [up, up, cut, cut],
        w_other, net_weight, i_other, i_own, cap_other, capacitance,
        hbm=range(2),
        scratch=[
            pltpu.VMEM((2, nodes, nets), F32), pltpu.SemaphoreType.DMA((2,)),
        ],
    )
    state = [((steps, wide), F32)] * 3
    landing = [pltpu.VMEM(*message), pltpu.SemaphoreType.DMA((1,))]
    aux_shape = (-(-(4 + 3 * levels) // SUB) * SUB, max(wide, 2 * channels))
    w, r, c, part, msg, aux = call(
        functools.partial(opening_kernel, plan, steps, channels, sections, doms, levels),
        state + [((steps, nets), F32), message, (aux_shape, F32)],
        spot, got, p_other, pack, ah, al, th, tl,
        hbm_outs=(4,),
        scratch=landing,
    )
    means = []
    taps = None
    bits = (doms // 2 - 1).bit_length()
    for index in range(1, NEWTON * SWEEPS):
        own = part
        recv = jnp.zeros_like(part) if bits == 0 else along_dom(own, 0)
        got = gather(msg)
        for bit in range(1, bits):
            own = own + recv
            recv = along_dom(own, bit)
        last = index == NEWTON * SWEEPS - 1
        (u,) = call(back_kernel, [((steps, wide), F32)], own, recv, r, th, tl)
        if last:
            break
        boundary = index % NEWTON == 0
        before = index % NEWTON == NEWTON - 1
        mode = "drive" if boundary else "taps" if before else "plain"
        extra = []
        if mode == "drive":
            prefix, total = jnp.zeros_like(taps), taps
            mix = aux[4 : 4 + 3 * levels, : 2 * channels]
            for level in range(levels):
                if sections == 1:
                    break
                got_taps = along_section(total, level)
                prefix = prefix + mix[3 * level + 2][None] * got_taps
                total = mix[3 * level][None] * total + mix[3 * level + 1][None] * got_taps
            extra = [prefix]
        outs = state + [((steps, nets), F32), message, ((1, LANES), F32)]
        if mode == "taps":
            outs = outs + [((2 * steps, 2 * channels), F32)]
        result = call(
            functools.partial(round_kernel, plan, steps, channels, cells, mode),
            outs,
            spot, got, u, w, r, c, ah, al, th, tl, aux, *extra,
            hbm_outs=(4,),
            scratch=landing,
        )
        w, r, c, part, msg, mean = result[:6]
        means.append(mean)
        if mode == "taps":
            taps = result[6]
    w, r, msg, mean = call(
        functools.partial(residual_kernel, cells),
        [((steps, wide), F32), ((steps, wide), F32), message, ((1, LANES), F32)],
        spot, got, u, w, r, c,
    )
    means.append(mean)
    got = gather(msg)
    w, c, give = call(
        functools.partial(correct_kernel, plan),
        [((steps, nodes), F32), ((steps, nodes), F32), ((2 * steps, nodes), F32)],
        w, r, ah, al,
    )
    given = swap(give)
    out, history = call(
        functools.partial(last_kernel, steps, cells),
        [((steps, nodes), F32), ((NEWTON * SWEEPS,), F32)],
        spot, got, w, c, given, *means,
    )
    return (out[None], history)


def solution(mesh):
    return jax.shard_map(
        per_device,
        mesh=mesh,
        in_specs=(
            P("section", None, "dom"),
            P("section", "dom"),
            P("section", "dom"),
            P("section", "dom", None, None),
            P("section", "dom", None, None),
            P("section", "dom", None),
            P("section", "dom"),
            P("section", "dom"),
            P("section", "dom"),
            P("section", "dom"),
        ),
        out_specs=(P("section", None, "dom"), P()),
        check_vma=False,
    )
```

```python
import functools

import jax
import jax.numpy as jnp
from jax import lax
from jax.experimental import pallas as pl
from jax.experimental.pallas import tpu as pltpu
from jax.sharding import PartitionSpec as P


NEWTON = 2
SWEEPS = 2
HIGHEST = lax.Precision.HIGHEST
F32 = jnp.float32
BF16 = jnp.bfloat16
LANES = 128
SUB = 8


def fdot(a, b):
    return jnp.dot(a, b, precision=HIGHEST, preferred_element_type=F32)


def bdot(a, b):
    return jnp.dot(a, b, preferred_element_type=F32)


def tdot(a, b):
    return lax.dot_general(a, b, (((1,), (1,)), ((), ())), preferred_element_type=F32)


def split(x):
    high = x.astype(BF16)
    return high, (x - high.astype(F32)).astype(BF16)


def dot3(x, high, low, dot):
    rows = x.shape[0]
    xh, xl = split(x)
    both = dot(jnp.concatenate([xh, xl], axis=0), high)
    return both[:rows] + both[rows:] + dot(xh, low)


def dot2(x, exact):
    rows = x.shape[0]
    xh, xl = split(x)
    both = bdot(jnp.concatenate([xh, xl], axis=0), exact)
    return both[:rows] + both[rows:]


def lag(x, offset):
    if offset == 0:
        return x
    if offset >= x.shape[0]:
        return jnp.zeros_like(x)
    if offset % SUB == 0:
        return jnp.concatenate([jnp.zeros((offset, x.shape[1]), F32), x[: x.shape[0] - offset]], axis=0)
    row = lax.broadcasted_iota(jnp.int32, x.shape, 0)
    return jnp.where(row >= offset, pltpu.roll(x, offset, 0), 0.0)


def stages(steps):
    plan = [(0, 1)]
    span = 2
    while span < steps:
        plan.append((span,))
        span *= 2
    return plan


def powers_of(plan):
    return [p for stage in plan[1:] for p in stage]


def tree(parts):
    while len(parts) > 1:
        parts = [parts[i] + parts[i + 1] if i + 1 < len(parts) else parts[i] for i in range(0, len(parts), 2)]
    return parts[0]


def tile_sum(x):
    return tree([x[i : i + SUB, j : j + LANES] for i in range(0, x.shape[0], SUB) for j in range(0, x.shape[1], LANES)])


def land(moves, sems):
    copies = [pltpu.make_async_copy(src, dst, sems.at[i]) for i, (src, dst) in enumerate(moves)]
    for copy in copies:
        copy.start()
    return copies


def first_kernel(initial, weight, tap, att, msg, b_initial, b_weight, b_tap, b_att, sems):
    nodes = initial.shape[1]
    channels = tap.shape[1]
    copies = land([(initial, b_initial), (tap, b_tap), (att, b_att), (weight, b_weight)], sems)
    for copy in copies[:3]:
        copy.wait()
    start = b_initial[...]
    node = lax.broadcasted_iota(jnp.int32, (nodes, channels), 0)
    taps = fdot(start, (node == b_tap[...]).astype(F32))
    copies[3].wait()
    net = fdot(start, b_weight[...])
    rows = []
    for j in range(0, net.shape[1], LANES):
        rows.append(net[:, j : j + LANES])
    for row in (taps, b_att[...]):
        for j in range(0, channels, LANES):
            rows.append(row[:, j : j + LANES])
    assert len(rows) <= SUB
    rows += [jnp.zeros((1, LANES), F32)] * (SUB - len(rows))
    tile = jnp.concatenate(rows, axis=0)
    msg[...] = jnp.broadcast_to(tile[None], msg.shape)


def pack_kernel(source, initial, capacitance, matrix, tap, drive, gain, inverse, pack, near_inverse,
                b_initial, b_capacitance, b_matrix, b_tap, b_drive, b_gain, sems):
    steps, nodes = source.shape
    blocks, width = matrix.shape[0], matrix.shape[1]
    channels = tap.shape[1]
    copies = land(
        [(initial, b_initial), (matrix, b_matrix), (capacitance, b_capacitance), (tap, b_tap), (drive, b_drive),
         (gain, b_gain), (source, pack.at[0:steps, :]), (inverse, near_inverse)],
        sems,
    )
    pack[steps : steps + SUB, :] = jnp.zeros((SUB, nodes), F32)
    for copy in copies:
        copy.wait()
    start = b_initial[...]
    parts = []
    for k in range(blocks):
        parts.append(
            lax.dot_general(
                start[:, k * width : (k + 1) * width],
                b_matrix[k],
                (((1,), (1,)), ((), ())),
                precision=HIGHEST,
                preferred_element_type=F32,
            )
        )
    held = jnp.concatenate(parts, axis=1) - b_capacitance[...] * start
    for i, row in enumerate((held, start, b_capacitance[...])):
        pack[steps + i : steps + i + 1, :] = row
    for i, row in enumerate((b_gain[...], b_tap[...].astype(F32), b_drive[...].astype(F32))):
        pack[steps + 3 + i : steps + 4 + i, 0:channels] = row


def both(ref_other, ref_own, lo, hi):
    return jnp.concatenate([ref_other[lo:hi, :], ref_own[lo:hi, :]], axis=1)


def prep_kernel(plan, w_other, w_own, i_other, i_own, cap_other, cap_own, wh, wl, ah, al, b_w, sems):
    nodes = w_own.shape[0]
    blocks, width = i_own.shape[0], i_own.shape[1]
    copies = land([(w_other, b_w.at[0]), (w_own, b_w.at[1])], sems)
    cap = jnp.concatenate([cap_other[...], cap_own[...]], axis=1)
    wanted = powers_of(plan)
    eye = lax.broadcasted_iota(jnp.int32, (width, width), 0) == lax.broadcasted_iota(jnp.int32, (width, width), 1)

    def times(x, y):
        return bdot(x[0], y[0]) + bdot(x[1], y[0]) + bdot(x[0], y[1])

    every = range(2 * blocks)
    inverse = [split((i_other if b < blocks else i_own)[b % blocks].T) for b in every]
    scale = [split(jnp.where(eye, cap[:, b * width : (b + 1) * width], 0.0)) for b in every]
    made = {1: [split(times(scale[b], inverse[b])) for b in every]}
    todo = [inverse, [split(times(inverse[b], made[1][b])) for b in every]]
    power = 2
    while power <= max(wanted):
        made[power] = [split(times(x, x)) for x in made[power // 2]]
        power *= 2
    for p in wanted:
        if p not in made:
            top = 1 << (p.bit_length() - 1)
            made[p] = [split(times(made[top][b], made[p - top][b])) for b in every]
        todo.append(made[p])
    for i, value in enumerate(todo):
        for b in every:
            here = slice(i * width, (i + 1) * width)
            ah[b, here, :], al[b, here, :] = value[b]
    for copy in copies:
        copy.wait()
    for half in range(2):
        here = slice(half * nodes, (half + 1) * nodes)
        h, l = split(b_w[half])
        wh[here, :] = h
        wl[here, :] = l


def march(plan, x, ah, al):
    blocks, width = ah.shape[0], ah.shape[2]
    rows = x.shape[0]
    unit = 0
    for s, stage in enumerate(plan):
        parts = [split(lag(x, offset)) for offset in stage]
        there = slice(unit * width, (unit + len(stage)) * width)
        unit += len(stage)
        sums = []
        for b in range(blocks):
            here = slice(b * width, (b + 1) * width)
            xh = jnp.concatenate([h[:, here] for h, _ in parts], axis=1)
            xl = jnp.concatenate([l[:, here] for _, l in parts], axis=1)
            two = bdot(jnp.concatenate([xh, xl], axis=0), ah[b, there, :])
            sums.append(two[:rows] + two[rows:] + bdot(xh, al[b, there, :]))
        total = jnp.concatenate(sums, axis=1)
        x = total if s == 0 else total + x
    return x


def send_squares(r, spot, msg):
    row = jnp.sum(tile_sum(r * r), axis=0, keepdims=True) * spot[2:3, :]
    msg[...] = jnp.broadcast_to(row, msg.shape)


def finish_round(plan, r, spot, r_ref, c_ref, p_ref, msg, ah, al, sent, wh, wl, more=None):
    near_msg, sem = sent
    r_ref[...] = r
    send_squares(r, spot, near_msg)
    leaving = pltpu.make_async_copy(near_msg, msg, sem.at[0])
    leaving.start()
    owner = jnp.max(spot[2:3, :]) > 0.5

    @pl.when(owner)
    def _():
        c = march(plan, r_ref[...], ah, al)
        c_ref[...] = c
        rows = c.shape[0]
        ch, cl = split(c)
        two = bdot(jnp.concatenate([ch, cl], axis=0), wh[...])
        p_ref[...] = two[:rows] + two[rows:] + bdot(ch, wl[...])
        if more is not None:
            more(c)

    @pl.when(jnp.logical_not(owner))
    def _():
        c_ref[...] = jnp.zeros_like(c_ref)
        p_ref[...] = jnp.zeros_like(p_ref)

    leaving.wait()


def opening_kernel(plan, steps, channels, sections, doms, levels, spot, got, p_other, p_own, ah, al, wh, wl,
                   w_ref, r_ref, c_ref, p_ref, msg, aux_ref, *sent):
    my, chip = spot[0:1, :], spot[1:2, :]
    nets = wh.shape[1]
    net_rows = nets // LANES
    tap_rows = channels // LANES
    mine = jnp.zeros((SUB, LANES), F32)
    for t in range(sections):
        whole = tree([got[t * doms + d] for d in range(doms)])
        mine = jnp.where(my == float(t), whole, mine)
    net = jnp.concatenate([mine[i : i + 1, :] for i in range(net_rows)], axis=1)

    tiles = []
    for t in range(sections):
        halves = []
        for half in range(2):
            tile = got[t * doms + half]
            for z in range(1, doms // 2):
                tile = jnp.where(chip == float(z), got[t * doms + 2 * z + half], tile)
            halves.append(tile)
        tiles.append(halves)

    def channel_row(s, first):
        pieces = []
        for half in range(2):
            pieces += [tiles[s][half][first + i : first + i + 1, :] for i in range(tap_rows)]
        return jnp.concatenate(pieces, axis=1)

    lanes = 2 * channels // LANES
    here = jnp.concatenate([my] * lanes, axis=1).astype(jnp.int32)
    decay, carried, drive = [], None, jnp.zeros((1, 2 * channels), F32)
    for s in range(sections):
        a = channel_row(s, net_rows + tap_rows)
        decay.append(a)
        if carried is not None:
            drive = jnp.where(here == s, carried, drive)
        tapped = channel_row(s, net_rows)
        carried = tapped if carried is None else a * carried + tapped
    one = jnp.ones((1, 2 * channels), F32)
    rows = []
    for level in range(levels):
        bit = (here >> level) & 1
        own_a, other_a, past_a = one, one, one
        for s in range(sections):
            up = s >> level
            own_a = jnp.where((here >> level) == up, own_a * decay[s], own_a)
            other_a = jnp.where(((here >> level) ^ 1) == up, other_a * decay[s], other_a)
            past_a = jnp.where(((here >> level) == up) & (here > s), past_a * decay[s], past_a)
        rows += [jnp.where(bit == 1, one, other_a), jnp.where(bit == 1, own_a, one), jnp.where(bit == 1, past_a, 0.0)]
    nodes = p_own.shape[1]
    kept = [
        jnp.concatenate([p_other[i : i + 1, 0:channels], p_own[i : i + 1, 0:channels]], axis=1)
        for i in (steps + 3, steps + 4, steps + 5)
    ]
    inj = spread(jnp.broadcast_to(drive * kept[0], (SUB, 2 * channels)), kept[2], nodes)[0:1]
    aux_ref[...] = jnp.zeros_like(aux_ref)
    aux_ref[0:1, 0 : inj.shape[1]] = inj
    for i, row in enumerate(kept + rows):
        aux_ref[1 + i : 2 + i, 0 : 2 * channels] = row
    back = dot3(jnp.broadcast_to(net, (SUB, nets)), wh[...], wl[...], tdot)[0:1]
    start = both(p_other, p_own, steps + 1, steps + 2)
    held = both(p_other, p_own, steps, steps + 1)
    q = (held + back - inj) - both(p_other, p_own, 0, steps)
    r = q + 0.5 * jnp.tanh(start)
    w_ref[...] = jnp.broadcast_to(start, w_ref.shape)
    finish_round(plan, r, spot, r_ref, c_ref, p_ref, msg, ah, al, sent, wh, wl)


def chosen(index, nodes):
    node = lax.broadcasted_iota(jnp.int32, (nodes, index.shape[1]), 0).astype(F32)
    return (node == index).astype(BF16)


def spread(drive, index, nodes):
    rows = drive.shape[0]
    channels = drive.shape[1] // 2
    out = []
    for h in range(2):
        here = slice(h * channels, (h + 1) * channels)
        xh, xl = split(drive[:, here])
        two = tdot(jnp.concatenate([xh, xl], axis=0), chosen(index[:, here], nodes))
        out.append(two[:rows] + two[rows:])
    return jnp.concatenate(out, axis=1)


def damping_of(got, cells):
    total = tile_sum(got[...])
    mean = jnp.sum(jnp.sum(total, axis=0, keepdims=True), axis=1, keepdims=True) / cells
    return mean, 1.0 / (1.0 + jnp.sqrt(mean))


def back_kernel(own, recv, r0, wh, wl, u_ref):
    u_ref[...] = r0[...] + dot3(own[...] + recv[...], wh[...], wl[...], tdot)


def advance(got, u, w0, r0, c0, cells, mean_ref):
    mean, damp = damping_of(got, cells)
    mean_ref[...] = jnp.broadcast_to(mean, mean_ref.shape)
    q0 = r0[...] - 0.5 * jnp.tanh(w0[...])
    return w0[...] - damp * c0[...], q0 - damp * u[...], damp


def round_kernel(plan, steps, channels, cells, mode, *refs):
    refs = list(refs)
    take = lambda n: [refs.pop(0) for _ in range(n)]
    (spot, got, u, w0, r0, c0, ah, al, wh, wl, aux) = take(11)
    if mode == "drive":
        (pre,) = take(1)
    w_ref, r_ref, c_ref, p_ref, msg, mean_ref = take(6)
    if mode == "taps":
        (tt_ref,) = take(1)
    sent = take(2)
    w, q, damp = advance(got, u, w0, r0, c0, cells, mean_ref)
    if mode == "drive":
        drive = pre[0:steps, :] - damp * pre[steps : 2 * steps, :]
        gain, _, driven = (aux[i : i + 1, 0 : 2 * channels] for i in (1, 2, 3))
        q = q - (spread(drive * gain, driven, w.shape[1] // 2) - aux[0:1, 0 : w.shape[1]])
    r = q + 0.5 * jnp.tanh(w)
    w_ref[...] = w
    half = w.shape[1] // 2

    def tap(c):
        for h in range(2):
            here = slice(h * half, (h + 1) * half)
            there = slice(h * channels, (h + 1) * channels)
            tapped = chosen(aux[2:3, there], half)
            tt_ref[:, there] = dot2(jnp.concatenate([w_ref[:, here], c[:, here]], axis=0), tapped)

    more = None
    if mode == "taps":
        more = tap
        tt_ref[...] = jnp.zeros_like(tt_ref)
    finish_round(plan, r, spot, r_ref, c_ref, p_ref, msg, ah, al, sent, wh, wl, more)


def residual_kernel(cells, spot, got, u, w0, r0, c0, w_ref, r_ref, msg, mean_ref):
    w, q, _ = advance(got, u, w0, r0, c0, cells, mean_ref)
    r = q + 0.5 * jnp.tanh(w)
    w_ref[...] = w
    r_ref[...] = r
    send_squares(r, spot, msg)


def correct_kernel(plan, w_in, r_in, ah, al, w_ref, c_ref, give):
    steps = r_in.shape[0]
    c = march(plan, r_in[...], ah, al)
    half = c.shape[1] // 2
    w = w_in[...]
    w_ref[...] = w[:, half:]
    c_ref[...] = c[:, half:]
    give[0:steps, :] = w[:, 0:half]
    give[steps : 2 * steps, :] = c[:, 0:half]


def last_kernel(steps, cells, spot, got, w, c, given, m1, m2, m3, out, means):
    mean, damp = damping_of(got, cells)
    north = jnp.concatenate([spot[2:3, :]] * (out.shape[1] // LANES), axis=1) == 1.0
    w_here = jnp.where(north, w[...], given[0:steps, :])
    c_here = jnp.where(north, c[...], given[steps : 2 * steps, :])
    out[...] = w_here - damp * c_here
    lane = lax.broadcasted_iota(jnp.int32, (1, LANES), 1)
    row = jnp.where(lane == 0, m1[...], jnp.where(lane == 1, m2[...], jnp.where(lane == 2, m3[...], mean)))
    means[...] = row[0, 0 : means.shape[0]]


def call(kernel, outs, *args, hbm=(), hbm_outs=(), scratch=()):
    def place(i, far):
        return pl.BlockSpec(memory_space=pltpu.HBM if i in far else pltpu.VMEM)

    args = [pltpu.with_memory_space_constraint(x, pltpu.HBM) if i in hbm else x for i, x in enumerate(args)]
    return pl.pallas_call(
        kernel,
        out_shape=[pltpu.HBM(s, d) if i in hbm_outs else jax.ShapeDtypeStruct(s, d) for i, (s, d) in enumerate(outs)],
        in_specs=[place(i, hbm) for i in range(len(args))],
        out_specs=[place(i, hbm_outs) for i in range(len(outs))],
        scratch_shapes=scratch,
        compiler_params=pltpu.CompilerParams(vmem_limit_bytes=16 << 20),
    )(*args)


def per_device(
    source,
    initial,
    capacitance,
    block_matrix,
    block_inverse,
    net_weight,
    tap_nodes,
    drive_nodes,
    drive_gain,
    attenuation,
):
    source = source[0]
    block_matrix = block_matrix[0]
    block_inverse = block_inverse[0]
    net_weight = net_weight[0]
    steps, nodes = source.shape
    blocks, width = block_matrix.shape[:2]
    nets = net_weight.shape[1]
    channels = tap_nodes.shape[1]
    sections, doms = lax.axis_size("section"), lax.axis_size("dom")
    devices = sections * doms
    everywhere = ("section", "dom")
    wide = 2 * nodes
    cells = float(devices * steps * nodes)
    plan = stages(steps)
    units = 2 + len(powers_of(plan))
    levels = max(1, (sections - 1).bit_length())

    def swap(x):
        return lax.ppermute(x, "dom", [(i, i ^ 1) for i in range(doms)])

    def pair(x, odd, even):
        links = []
        for s in range(sections):
            for d in range(doms):
                ps, pd = odd(s, d) if d % 2 else even(s, d)
                links.append((s * doms + d, ps * doms + pd))
        return lax.ppermute(x, everywhere, links)

    def along_dom(x, bit):
        return pair(x, lambda s, d: (s, d ^ (2 << bit)), lambda s, d: (s ^ 1, d))

    def along_section(x, bit):
        return pair(x, lambda s, d: (s ^ (1 << bit), d), lambda s, d: (s, d ^ 2))

    def gather(msg):
        spread_out = msg.reshape((devices, -1, LANES))
        return lax.all_to_all(spread_out, everywhere, 0, 0, tiled=False).reshape(msg.shape)

    core = lax.axis_index("dom")
    spot = jnp.stack([lax.axis_index("section"), core // 2, core % 2] + [core] * 5).astype(F32)
    spot = jnp.broadcast_to(spot[:, None], (SUB, LANES))
    w_other = swap(net_weight)
    i_other = swap(block_inverse)
    cap_other = swap(capacitance)
    first_message = ((devices, SUB, LANES), F32)
    message = ((devices, LANES), F32)
    row = lambda n, d=F32: pltpu.VMEM((1, n), d)
    (msg,) = call(
        first_kernel,
        [first_message],
        initial, net_weight, tap_nodes, attenuation,
        hbm=range(4),
        scratch=[
            row(nodes), pltpu.VMEM(net_weight.shape, F32), row(channels, jnp.int32), row(channels),
            pltpu.SemaphoreType.DMA((4,)),
        ],
    )
    got = gather(msg)
    pack, i_own = call(
        pack_kernel,
        [((steps + SUB, nodes), F32), (block_inverse.shape, F32)],
        source, initial, capacitance, block_matrix, tap_nodes, drive_nodes, drive_gain, block_inverse,
        hbm=range(8),
        scratch=[
            row(nodes), row(nodes), pltpu.VMEM(block_matrix.shape, F32),
            row(channels, jnp.int32), row(channels, jnp.int32), row(channels), pltpu.SemaphoreType.DMA((8,)),
        ],
    )
    p_other = swap(pack)
    cut = ((2 * blocks, units * width, width), BF16)
    up = ((wide, nets), BF16)
    wh, wl, ah, al = call(
        functools.partial(prep_kernel, plan),
        [up, up, cut, cut],
        w_other, net_weight, i_other, i_own, cap_other, capacitance,
        hbm=range(2),
        scratch=[
            pltpu.VMEM((2, nodes, nets), F32), pltpu.SemaphoreType.DMA((2,)),
        ],
    )
    state = [((steps, wide), F32)] * 3
    landing = [pltpu.VMEM(*message), pltpu.SemaphoreType.DMA((1,))]
    aux_shape = (-(-(4 + 3 * levels) // SUB) * SUB, max(wide, 2 * channels))
    w, r, c, part, msg, aux = call(
        functools.partial(opening_kernel, plan, steps, channels, sections, doms, levels),
        state + [((steps, nets), F32), message, (aux_shape, F32)],
        spot, got, p_other, pack, ah, al, wh, wl,
        hbm_outs=(4,),
        scratch=landing,
    )
    means = []
    taps = None
    bits = (doms // 2 - 1).bit_length()
    for index in range(1, NEWTON * SWEEPS):
        own = part
        recv = jnp.zeros_like(part) if bits == 0 else along_dom(own, 0)
        got = gather(msg)
        for bit in range(1, bits):
            own = own + recv
            recv = along_dom(own, bit)
        last = index == NEWTON * SWEEPS - 1
        (u,) = call(back_kernel, [((steps, wide), F32)], own, recv, r, wh, wl)
        if last:
            break
        boundary = index % NEWTON == 0
        before = index % NEWTON == NEWTON - 1
        mode = "drive" if boundary else "taps" if before else "plain"
        extra = []
        if mode == "drive":
            prefix, total = jnp.zeros_like(taps), taps
            mix = aux[4 : 4 + 3 * levels, : 2 * channels]
            for level in range(levels):
                if sections == 1:
                    break
                got_taps = along_section(total, level)
                prefix = prefix + mix[3 * level + 2][None] * got_taps
                total = mix[3 * level][None] * total + mix[3 * level + 1][None] * got_taps
            extra = [prefix]
        outs = state + [((steps, nets), F32), message, ((1, LANES), F32)]
        if mode == "taps":
            outs = outs + [((2 * steps, 2 * channels), F32)]
        result = call(
            functools.partial(round_kernel, plan, steps, channels, cells, mode),
            outs,
            spot, got, u, w, r, c, ah, al, wh, wl, aux, *extra,
            hbm_outs=(4,),
            scratch=landing,
        )
        w, r, c, part, msg, mean = result[:6]
        means.append(mean)
        if mode == "taps":
            taps = result[6]
    w, r, msg, mean = call(
        functools.partial(residual_kernel, cells),
        [((steps, wide), F32), ((steps, wide), F32), message, ((1, LANES), F32)],
        spot, got, u, w, r, c,
    )
    means.append(mean)
    got = gather(msg)
    w, c, give = call(
        functools.partial(correct_kernel, plan),
        [((steps, nodes), F32), ((steps, nodes), F32), ((2 * steps, nodes), F32)],
        w, r, ah, al,
    )
    given = swap(give)
    out, history = call(
        functools.partial(last_kernel, steps, cells),
        [((steps, nodes), F32), ((NEWTON * SWEEPS,), F32)],
        spot, got, w, c, given, *means,
    )
    return (out[None], history)


def solution(mesh):
    return jax.shard_map(
        per_device,
        mesh=mesh,
        in_specs=(
            P("section", None, "dom"),
            P("section", "dom"),
            P("section", "dom"),
            P("section", "dom", None, None),
            P("section", "dom", None, None),
            P("section", "dom", None),
            P("section", "dom"),
            P("section", "dom"),
            P("section", "dom"),
            P("section", "dom"),
        ),
        out_specs=(P("section", None, "dom"), P()),
        check_vma=False,
    )
```
